256 devices in a mesh: cfg: 2 (over z), space: 64 (over x, y), tm: 2 (over core).
Axes of the slice: x: 8, y: 8, z: 2, core: 2. Of those that a mesh axis runs over, the one named last changes fastest.
The devices are a block of a 8x8x16 slice.
Arguments:
- vectors: bfloat16 [4, 64, 6, 65536], P(('cfg', 'tm'), 'space'), parts along dimension 0, may hold values from -0.625 to 0.625
- gauge_links: bfloat16 [4, 3, 18, 65536], P(('cfg', 'tm'), None, None, 'space'), parts along dimension 0, may hold values from -3 to 3
- momenta: int32 [8, 3], replicated, may hold values from -2 to 2
- directions: int32 [3], replicated, may hold values from 0 to 2, each once
Outputs:
- elementals: float32 [64, 4, 8, 3, 128], P('space', ('cfg', 'tm')), parts along dimension 1
The draws below stay inside these ranges and needn't reach their ends.
There are 2 independent parts, one for each index of `cfg`. The reference program is written for one: setup_inputs(seed, part) draws one part's arguments, and reference() takes and returns one part's arrays. A program takes and returns all parts, laid end to end along the dimension named above; an argument that names none is the same for every part. Nothing has to cross between parts.
Inputs may be any that keep to these rules, and one draw needn't show every extreme that they name: `momenta`: integer momentum components, in units of 2 pi over the lattice extent. Each of the directions 0, 1, 2 appears once.
All inputs are finite; a program needn't handle non-finite values.
Results may differ from the reference program's by a relative error of at most 0.005.
Values may be sent and summed in bfloat16 or wider, within the bound.
A program may use at most 128 MiB of HBM per device.

```python
import math
import jax
import jax.numpy as jnp
from jax import lax

NEV = 64
LXY = 32
NMOM = 8
NDIR = 3
LZ = 64
SITES = 65536
T_SIZE = 2


def place_ends(drawn, key, least, high):
    longest = drawn.shape.index(max(drawn.shape))
    spots = []
    for shift in (0, 1):
        where = [jax.random.randint(jax.random.fold_in(key, axis), (), 0, length) for axis, length in enumerate(drawn.shape)]
        where[longest] = (where[longest] + shift) % drawn.shape[longest]
        spots.append(tuple(where))
    return drawn.at[spots[0]].set(least).at[spots[1]].set(high)


def with_spikes(values, stream_key, source, target, blocks, factor):
    owner, partner = [(jnp.arange(values.shape[position]) // (values.shape[position] // blocks)).reshape([-1 if axis == position else 1 for axis in range(values.ndim)]) for position in (source, target)]
    chosen = jax.random.permutation(stream_key, blocks)[partner]
    strong = (owner == chosen) | (owner == (partner + blocks // 2) % blocks)
    return jnp.where(strong, factor * values, values)


def level_of(key, extent, shards, smallest, top_value):
    factor_of, own = 1.0, jax.random.fold_in(key, 6)
    for axis_at, shards_of in shards:
        heights = jnp.exp(jax.random.uniform(jax.random.fold_in(own, axis_at), (shards_of,), jnp.float32, smallest / len(shards), top_value / len(shards)))
        factor_of = factor_of * jnp.repeat(heights, extent[axis_at] // shards_of).reshape([-1 if axis == axis_at else 1 for axis in range(len(extent))])
    return factor_of


def centred(rng, dims, scale, most, split=(), kind=jnp.bfloat16):
    level = level_of(rng, dims, split, -0.22, 0.18) if split else 1.0
    entries = jax.random.normal(rng, dims, jnp.float32) * scale * level
    return jnp.minimum(jnp.maximum(entries, -most), most).astype(kind)


def noise_with(own_key, extent, spread, most, cuts, heavy, kind=jnp.bfloat16):
    values = spread * jax.random.normal(own_key, extent, jnp.float32)
    if cuts:
        values = values * level_of(own_key, extent, cuts, -0.22, 0.18)
    return jnp.clip(with_spikes(values, jax.random.fold_in(own_key, 3), *heavy), -most, most).astype(kind)


def setup_inputs(seed: int = 0, part: int = 0) -> dict:
    arg_keys = jax.random.split(jax.random.key(seed), 5)
    part_keys = jax.random.split(jax.random.fold_in(arg_keys[4], part), 5)
    vectors = noise_with(part_keys[0], (T_SIZE, NEV, 6, SITES), ((6 * SITES) ** -0.25), 0.625, ((0, 2), (1, 64)), (3, 1, 64, 4.0))
    gauge_links = centred(part_keys[1], (T_SIZE, 3, 18, SITES), 0.5, 3.0, ((0, 2), (3, 64)))
    momenta = place_ends(jax.random.randint(arg_keys[2], (NMOM, 3), -2, 3), jax.random.fold_in(arg_keys[2], 1), -2, 2).astype(jnp.int32)
    directions = jax.random.permutation(arg_keys[3], 3).astype(jnp.int32)
    return dict(vectors=vectors, gauge_links=gauge_links, momenta=momenta, directions=directions)


TWO_PI = 2.0 * math.pi


def apply_link(link, field_f32):
    real_rows = []
    imag_rows = []
    for row_a in range(3):
        link_re = link[0, row_a, 0][None]
        link_im = link[1, row_a, 0][None]
        real_acc = link_re * field_f32[:, 0, 0] - link_im * field_f32[:, 1, 0]
        imag_acc = link_re * field_f32[:, 1, 0] + link_im * field_f32[:, 0, 0]
        for col_b in range(1, 3):
            link_re = link[0, row_a, col_b][None]
            link_im = link[1, row_a, col_b][None]
            real_acc = real_acc + link_re * field_f32[:, 0, col_b] - link_im * field_f32[:, 1, col_b]
            imag_acc = imag_acc + link_re * field_f32[:, 1, col_b] + link_im * field_f32[:, 0, col_b]
        real_rows.append(real_acc)
        imag_rows.append(imag_acc)
    return jnp.stack([jnp.stack(real_rows, axis=1), jnp.stack(imag_rows, axis=1)], axis=1)


def adjoint(link):
    return jnp.stack([jnp.swapaxes(link[0], 0, 1), -jnp.swapaxes(link[1], 0, 1)])


def pack_terms(derivative, eig_count):
    rounded = derivative.astype(jnp.bfloat16)
    rounded_re = rounded[:, 0]
    rounded_im = rounded[:, 1]
    swapped = jnp.stack([rounded_im, -rounded_re], axis=1)
    return jnp.concatenate([rounded, swapped], axis=0).reshape(2 * eig_count, -1)


def phase_angles(momenta, z_offset, depth_planes, z_length):
    z_coord = (z_offset + jnp.arange(depth_planes, dtype=jnp.int32)).astype(jnp.int32)
    y_coord = jnp.arange(LXY, dtype=jnp.int32)
    x_coord = jnp.arange(LXY, dtype=jnp.int32)
    mom_x = momenta[:, 0][:, None, None, None]
    mom_y = momenta[:, 1][:, None, None, None]
    mom_z = momenta[:, 2][:, None, None, None]
    fraction = ((mom_x * x_coord[None, None, None, :]) % LXY).astype(jnp.float32) / LXY
    fraction = fraction + ((mom_y * y_coord[None, None, :, None]) % LXY).astype(jnp.float32) / LXY
    fraction = fraction + ((mom_z * z_coord[None, :, None, None]) % z_length).astype(jnp.float32) / z_length
    return TWO_PI * fraction


def phase_twist(row_block, cosine_table, sine_table):
    vec_re = row_block[:, 0][None]
    vec_im = row_block[:, 1][None]
    cos_b = cosine_table[:, None, None]
    sin_b = sine_table[:, None, None]
    real_part = vec_re * cos_b - vec_im * sin_b
    imag_part = vec_re * sin_b + vec_im * cos_b
    twisted = jnp.stack([real_part, imag_part], axis=2).astype(jnp.bfloat16)
    return twisted.reshape(cosine_table.shape[0] * row_block.shape[0], -1)


def reference(vectors, gauge_links, momenta, directions):
    slab_count = vectors.shape[0]
    eig_count = vectors.shape[1]
    angles = phase_angles(momenta, 0, LZ, LZ)
    cosine_all = jnp.cos(angles)
    sine_all = jnp.sin(angles)
    per_slab = []
    for slab in range(slab_count):
        field_f32 = vectors[slab].reshape(eig_count, 2, 3, LZ, LXY, LXY).astype(jnp.float32)
        slab_links = gauge_links[slab].reshape(3, 2, 3, 3, LZ, LXY, LXY).astype(jnp.float32)
        packed_list = []
        for dir_index, roll_axis in ((0, -1), (1, -2), (2, -3)):
            forward = apply_link(slab_links[dir_index], jnp.roll(field_f32, -1, axis=roll_axis))
            backward = jnp.roll(apply_link(adjoint(slab_links[dir_index]), field_f32), 1, axis=roll_axis)
            packed_list.append(pack_terms(0.5 * (forward - backward), eig_count))
        packed_all = jnp.stack(packed_list)
        per_mom = []
        for mom_index in range(NMOM):
            twisted = phase_twist(field_f32, cosine_all[mom_index:mom_index + 1], sine_all[mom_index:mom_index + 1]).astype(jnp.float32)
            per_dir = []
            for dir_slot in range(NDIR):
                chosen = packed_all[directions[dir_slot]].astype(jnp.float32)
                per_dir.append(jnp.dot(twisted, chosen.T, precision=lax.Precision.HIGHEST))
            per_mom.append(jnp.stack(per_dir, axis=1))
        per_slab.append(jnp.stack(per_mom, axis=1))
    return jnp.stack(per_slab, axis=1)
```

```python
import functools
import math

import jax
import jax.numpy as jnp
from jax import lax
from jax.experimental import pallas as pl
from jax.experimental.pallas import tpu as pltpu
from jax.sharding import PartitionSpec as P

LXY = 32
NMOM = 8
NDIR = 3
PLANE = LXY * LXY
LANES = 128
BLOCKS = PLANE // LANES
HALF = PLANE // 2
COMPS = 6
BLOCK_ROWS = COMPS * BLOCKS
PITCH = BLOCK_ROWS + 8
GROUP = 16
TWO_PI = 2.0 * math.pi
MESH = pl.DeviceIdType.MESH


def phase_tables(momenta, plane, z_length):
    sites = jnp.arange(PLANE, dtype=jnp.int32)
    x_coord, y_coord = sites % LXY, sites // LXY
    halo = jnp.where(sites < HALF, plane + 1, plane - 1) % z_length
    z_coord = jnp.stack([jnp.full_like(sites, plane), halo])
    fraction = ((momenta[:, 0:1] * x_coord[None]) % LXY).astype(jnp.float32) / LXY
    fraction = fraction + ((momenta[:, 1:2] * y_coord[None]) % LXY).astype(jnp.float32) / LXY
    along_z = (momenta[None, :, 2:3] * z_coord[:, None, :]) % z_length
    theta = TWO_PI * (fraction[None] + along_z.astype(jnp.float32) / z_length)
    return jnp.cos(theta), jnp.sin(theta)


def roll(value, shift):
    return pltpu.roll(value, shift, value.ndim - 1)


def apply_table(table, lanes, field):
    out_re, out_im = [], []
    for row in range(3):
        acc_re = acc_im = None
        for col in range(3):
            link_re = table[3 * row + col : 3 * row + col + 1, lanes]
            link_im = table[9 + 3 * row + col : 10 + 3 * row + col, lanes]
            re = link_re * field[col] - link_im * field[3 + col]
            im = link_re * field[3 + col] + link_im * field[col]
            acc_re = re if acc_re is None else acc_re + re
            acc_im = im if acc_im is None else acc_im + im
        out_re.append(acc_re)
        out_im.append(acc_im)
    return out_re + out_im


def minus_adjoint(entries):
    real = [-entries[3 * b + a] for a in range(3) for b in range(3)]
    imag = [entries[9 + 3 * b + a] for a in range(3) for b in range(3)]
    return real + imag


def store_packed(packed, base, nev, rows_at, lanes, value):
    for colour in range(3):
        re = value[colour].astype(jnp.bfloat16)
        im = value[3 + colour].astype(jnp.bfloat16)
        packed[colour, pl.ds(base + rows_at, GROUP), lanes] = re
        packed[colour, pl.ds(base + nev + rows_at, GROUP), lanes] = im
        packed[3 + colour, pl.ds(base + rows_at, GROUP), lanes] = im
        packed[3 + colour, pl.ds(base + nev + rows_at, GROUP), lanes] = -re


def store_twisted(twisted, nev, rows_at, lanes, cosine, sine, field):
    for mom in range(NMOM):
        cos_row = cosine[mom : mom + 1, lanes]
        sin_row = sine[mom : mom + 1, lanes]
        for colour in range(3):
            vec_re, vec_im = field[colour], field[3 + colour]
            rows = pl.ds(mom * nev + rows_at, GROUP)
            twisted[colour, rows, lanes] = (vec_re * cos_row - vec_im * sin_row).astype(
                jnp.bfloat16
            )
            twisted[3 + colour, rows, lanes] = (vec_re * sin_row + vec_im * cos_row).astype(
                jnp.bfloat16
            )


def accumulate(acc, pairs):
    acc[...] = jnp.zeros_like(acc)
    for left, right in pairs:

        @pl.loop(0, COMPS)
        def _(slot):
            acc[...] += lax.dot_general(
                left[slot], right[slot], (((1,), (1,)), ((), ())),
                preferred_element_type=jnp.float32,
            )


def wait_for(ref, sem):
    pltpu.make_async_copy(ref, ref, sem).wait()


def kernel(
    side, groups, x_ref, links_ref, cos_ref, sin_ref, out_ref,
    ra, rb, spread, field, field_b, halo, links, links_z, table, twisted, twisted_h,
    packed_xy, packed_z, packed_h, acc_xy, acc_z, send_xy, send_z, got_xy, got_z,
    sum_xy, sum_z, rows_out, rows_in,
    sem_a, sem_b, sem_h, sem_l, sem_r, sem_s,
):
    nev = side * side
    me, core = lax.axis_index("space"), lax.axis_index("tm")
    high, low = me // side, me % side
    a = low + core * (high - low)
    b = high + core * (low - high)

    def device(at_a, at_b):
        return (1 - core) * (at_b * side + at_a) + core * (at_a * side + at_b)

    def device_of(plane):
        return device(plane % side, plane // side)

    plane = b * side + a
    above = device_of((plane + 1) % nev)
    below = device_of((plane + nev - 1) % nev)
    mirror = device_of(me)
    links_to = device_of((me + 1) % nev)
    links_from = (plane + nev - 1) % nev

    barrier = pltpu.get_barrier_semaphore()

    def greet(target):
        pl.semaphore_signal(barrier, inc=1, device_id={"space": target}, device_id_type=MESH)

    for step in range(1, side):
        greet(device((a + step) % side, b))
        greet(device(a, (b + step) % side))
    for target in (above, below, links_to, links_from):
        greet(target)

    @pl.when(mirror != me)
    def _():
        greet(mirror)
        pl.semaphore_wait(barrier, 2 * (side - 1) + 5)

    @pl.when(mirror == me)
    def _():
        pl.semaphore_wait(barrier, 2 * (side - 1) + 4)

    def send(src, dst, sent, arrived, target):
        copy = pltpu.make_async_remote_copy(
            src_ref=src, dst_ref=dst, send_sem=sent, recv_sem=arrived,
            device_id={"space": target}, device_id_type=MESH,
        )
        copy.start()
        return copy

    @pl.when(mirror != me)
    def _():
        send(links_ref, links, sem_s.at[0], sem_l.at[0], mirror)

    @pl.when(mirror == me)
    def _():
        pltpu.make_async_copy(links_ref, links, sem_l.at[0]).start()

    upper = pl.ds(HALF, HALF)
    links_copy = send(
        links_ref.at[2, :, upper], links_z, sem_s.at[1], sem_l.at[1], links_to
    )

    order_a = sorted(range(1, side), key=lambda k: -min(k, side - k))
    for index, group in enumerate(groups):
        for step_b in group:
            to_b = (b + step_b) % side
            for step_a in order_a:
                to_a = (a + step_a) % side
                send(
                    x_ref.at[to_a, to_b], ra.at[a, to_b], sem_s.at[2], sem_a.at[index],
                    device(to_a, b),
                )
    ra[a] = x_ref[a]

    wait_for(links, sem_l.at[0])
    links_copy.wait()
    lane = lax.broadcasted_iota(jnp.int32, (1, LANES), 1)
    x_lane = lane % LXY

    def block(index):
        return slice(index * LANES, (index + 1) * LANES)

    for direction in range(2):
        for at in range(BLOCKS):
            own = [
                0.5 * links[direction, e : e + 1, block(at)].astype(jnp.float32)
                for e in range(18)
            ]
            if direction == 0:
                moved = [jnp.where(x_lane == 0, roll(u, 97), roll(u, 1)) for u in own]
            else:
                before = (at + BLOCKS - 1) % BLOCKS
                other = [
                    0.5 * links[direction, e : e + 1, block(before)].astype(jnp.float32)
                    for e in range(18)
                ]
                moved = [
                    jnp.where(lane < LXY, roll(o, LXY), roll(u, LXY)) for o, u in zip(other, own)
                ]
            for e in range(18):
                table[2 * direction, e : e + 1, block(at)] = own[e]
            for e, value in enumerate(minus_adjoint(moved)):
                table[2 * direction + 1, e : e + 1, block(at)] = value
    low_half, high_half = slice(0, HALF), slice(HALF, PLANE)
    own = [0.5 * links[2, e : e + 1, low_half].astype(jnp.float32) for e in range(18)]
    lower = [0.5 * links_z[e : e + 1, :].astype(jnp.float32) for e in range(18)]
    for e in range(18):
        table[4, e : e + 1, low_half] = own[e]
        table[5, e : e + 1, high_half] = lower[e]
    for e, value in enumerate(minus_adjoint(own)):
        table[5, e : e + 1, low_half] = value
    for e, value in enumerate(minus_adjoint(lower)):
        table[4, e : e + 1, high_half] = value

    for index, group in enumerate(groups):
        wait_for(ra.at[pl.ds(0, side - 1), pl.ds(0, len(group))], sem_a.at[index])
        for step_b in group:
            to_b = (b + step_b) % side
            if step_b:
                send(ra.at[:, to_b], rb.at[:, b], sem_s.at[3], sem_b, device(a, to_b))
            else:
                for from_a in range(side):
                    rb[from_a, b] = ra[from_a, b]
    wait_for(rb.at[pl.ds(0, side - 1)], sem_b)

    @pl.loop(0, side)
    def _(from_a):
        for from_b in range(side):
            spread[pl.ds((from_a * side + from_b) * PITCH, BLOCK_ROWS), :] = rb[
                from_a, from_b
            ].astype(jnp.float32)

    @pl.loop(0, COMPS)
    def _(comp):
        for at in range(BLOCKS):
            rows = spread[pl.ds(comp * BLOCKS + at, nev, stride=PITCH), :]
            field[comp, :, block(at)] = rows
            field_b[comp, :, block(at)] = rows.astype(jnp.bfloat16)

    lower_half = pl.ds(0, HALF)
    down = send(
        field_b.at[:, :, lower_half], halo.at[:, :, lower_half], sem_s.at[4], sem_h.at[0], below
    )
    up = send(field_b.at[:, :, upper], halo.at[:, :, upper], sem_s.at[5], sem_h.at[1], above)

    @pl.loop(0, (nev // GROUP) * BLOCKS)
    def _(step):
        at = step % BLOCKS
        rows_at = pl.multiple_of((step // BLOCKS) * GROUP, GROUP)

        def lanes_of(index):
            return pl.ds(pl.multiple_of(index * LANES, LANES), LANES)

        lanes = lanes_of(at)
        after = lanes_of((at + 1) % BLOCKS)
        before = lanes_of((at + BLOCKS - 1) % BLOCKS)
        rows = pl.ds(rows_at, GROUP)
        vec = [field[c, rows, lanes] for c in range(COMPS)]
        store_twisted(twisted, nev, rows_at, lanes, cos_ref.at[0], sin_ref.at[0], vec)
        ahead = [jnp.where(x_lane == LXY - 1, roll(v, 31), roll(v, 127)) for v in vec]
        behind = [jnp.where(x_lane == 0, roll(v, 97), roll(v, 1)) for v in vec]
        first = apply_table(table.at[0], lanes, ahead)
        second = apply_table(table.at[1], lanes, behind)
        store_packed(packed_xy, 0, nev, rows_at, lanes, [f + s for f, s in zip(first, second)])
        ahead = [
            jnp.where(lane < LANES - LXY, roll(v, 96), roll(field[c, rows, after], 96))
            for c, v in enumerate(vec)
        ]
        behind = [
            jnp.where(lane < LXY, roll(field[c, rows, before], LXY), roll(v, LXY))
            for c, v in enumerate(vec)
        ]
        first = apply_table(table.at[2], lanes, ahead)
        second = apply_table(table.at[3], lanes, behind)
        store_packed(
            packed_xy, 2 * nev, nev, rows_at, lanes, [f + s for f, s in zip(first, second)]
        )
        store_packed(packed_h, 0, nev, rows_at, lanes, apply_table(table.at[5], lanes, vec))

    accumulate(acc_xy, [(twisted, packed_xy)])

    def spread_sums(acc, outgoing, got, parts, sem):
        width = parts * side
        for to_a in range(side):
            for mom in range(NMOM):
                tile = acc[mom * nev + to_a * side : mom * nev + (to_a + 1) * side, :]
                for part in range(parts):
                    at = mom * width + part * side
                    outgoing[to_a, at : at + side, :] = tile[
                        :, part * 2 * nev : (part + 1) * 2 * nev
                    ].astype(jnp.bfloat16)
        for step in order_a:
            to_a = (a + step) % side
            send(outgoing.at[to_a], got.at[step - 1], sem_s.at[5 + parts], sem, device(to_a, b))

    def collect_sums(outgoing, got, total, sem):
        wait_for(got, sem)
        value = outgoing[a].astype(jnp.float32)
        for index in range(side - 1):
            value = value + got[index].astype(jnp.float32)
        total[...] = value

    spread_sums(acc_xy, send_xy, got_xy, 2, sem_r.at[0])

    wait_for(halo.at[:, :, lower_half], sem_h.at[0])
    wait_for(halo.at[:, :, upper], sem_h.at[1])

    @pl.loop(0, (nev // GROUP) * BLOCKS)
    def _(step):
        rows_at = pl.multiple_of((step // BLOCKS) * GROUP, GROUP)
        lanes = pl.ds(pl.multiple_of((step % BLOCKS) * LANES, LANES), LANES)
        vec = [
            halo[c, pl.ds(rows_at, GROUP), lanes].astype(jnp.float32) for c in range(COMPS)
        ]
        store_twisted(twisted_h, nev, rows_at, lanes, cos_ref.at[1], sin_ref.at[1], vec)
        store_packed(packed_z, 0, nev, rows_at, lanes, apply_table(table.at[4], lanes, vec))

    accumulate(acc_z, [(twisted, packed_z), (twisted_h, packed_h)])
    spread_sums(acc_z, send_z, got_z, 1, sem_r.at[1])

    collect_sums(send_xy, got_xy, sum_xy, sem_r.at[0])
    collect_sums(send_z, got_z, sum_z, sem_r.at[1])
    for to_b in range(side):
        rows_out[to_b, 0 : 2 * NMOM, :] = sum_xy[pl.ds(to_b, 2 * NMOM, stride=side), :]
        rows_out[to_b, 2 * NMOM :, :] = sum_z[pl.ds(to_b, NMOM, stride=side), :]
    order_b = order_a
    for step in order_b:
        to_b = (b + step) % side
        send(rows_out.at[to_b], rows_in.at[step - 1], sem_s.at[8], sem_r.at[2], device(a, to_b))
    wait_for(rows_in, sem_r.at[2])
    value = rows_out[b]
    for index in range(side - 1):
        value = value + rows_in[index]
    out_ref[...] = value

    wait_for(ra.at[pl.ds(0, side - 1)], sem_s.at[2])
    wait_for(rb.at[pl.ds(0, side - 1)], sem_s.at[3])
    down.wait_send()
    up.wait_send()
    wait_for(got_z, sem_s.at[6])
    wait_for(got_xy, sem_s.at[7])
    wait_for(rows_in, sem_s.at[8])

    @pl.when(mirror != me)
    def _():
        wait_for(links, sem_s.at[0])


def shards(vectors, gauge_links, momenta, directions):
    space = lax.axis_size("space")
    side = math.isqrt(space)
    nev = space
    me, core = lax.axis_index("space"), lax.axis_index("tm")
    high, low = me // side, me % side
    plane = jnp.where(core == 0, me, low * side + high)
    blocks = vectors.reshape(COMPS, side, side, BLOCKS, LANES)
    blocks = jnp.transpose(blocks, (2, 1, 0, 3, 4)).reshape(side, side, BLOCK_ROWS, LANES)
    cosine, sine = phase_tables(momenta, plane, space)
    order = sorted(range(1, side), key=lambda k: -min(k, side - k)) + [0]
    cut = side // 2
    groups = (tuple(order[:cut]), tuple(order[cut:]))
    bf16, f32 = jnp.bfloat16, jnp.float32
    scratch = [
        ((side, side, BLOCK_ROWS, LANES), bf16),
        ((side, side, BLOCK_ROWS, LANES), bf16),
        ((nev * PITCH, LANES), f32),
        ((COMPS, nev, PLANE), f32),
        ((COMPS, nev, PLANE), bf16),
        ((COMPS, nev, PLANE), bf16),
        ((3, 18, PLANE), bf16),
        ((18, HALF), bf16),
        ((6, 24, PLANE), f32),
        ((COMPS, NMOM * nev, PLANE), bf16),
        ((COMPS, NMOM * nev, PLANE), bf16),
        ((COMPS, 4 * nev, PLANE), bf16),
        ((COMPS, 2 * nev, PLANE), bf16),
        ((COMPS, 2 * nev, PLANE), bf16),
        ((NMOM * nev, 4 * nev), f32),
        ((NMOM * nev, 2 * nev), f32),
        ((side, 2 * NMOM * side, 2 * nev), bf16),
        ((side, NMOM * side, 2 * nev), bf16),
        ((side - 1, 2 * NMOM * side, 2 * nev), bf16),
        ((side - 1, NMOM * side, 2 * nev), bf16),
        ((2 * NMOM * side, 2 * nev), f32),
        ((NMOM * side, 2 * nev), f32),
        ((side, NDIR * NMOM, 2 * nev), f32),
        ((side - 1, NDIR * NMOM, 2 * nev), f32),
    ]
    dma = pltpu.SemaphoreType.DMA
    out = pl.pallas_call(
        functools.partial(kernel, side, groups),
        out_shape=jax.ShapeDtypeStruct((NDIR * NMOM, 2 * nev), f32),
        in_specs=[
            pl.BlockSpec(memory_space=pltpu.VMEM),
            pl.BlockSpec(memory_space=pl.ANY),
            pl.BlockSpec(memory_space=pltpu.VMEM),
            pl.BlockSpec(memory_space=pltpu.VMEM),
        ],
        out_specs=pl.BlockSpec(memory_space=pltpu.VMEM),
        scratch_shapes=[pltpu.VMEM(*s) for s in scratch]
        + [dma((len(groups),)), dma, dma((2,)), dma((2,)), dma((3,)), dma((9,))],
        compiler_params=pltpu.CompilerParams(
            collective_id=0, has_side_effects=True, vmem_limit_bytes=60 * 1024 * 1024
        ),
    )(blocks, gauge_links[0], cosine, sine)
    by_dir = jnp.concatenate(
        [out[: 2 * NMOM].reshape(NMOM, 2, -1), out[2 * NMOM :].reshape(NMOM, 1, -1)], axis=1
    )
    square = by_dir.reshape(NMOM, NDIR, 2, side, side)
    square = jnp.where(core == 0, jnp.swapaxes(square, 3, 4), square)
    by_dir = square.reshape(NMOM, NDIR, 2 * nev)
    picked = [
        jnp.where(
            directions[d] == 0,
            by_dir[:, 0],
            jnp.where(directions[d] == 1, by_dir[:, 1], by_dir[:, 2]),
        )
        for d in range(NDIR)
    ]
    return jnp.stack(picked, axis=1)[None, None]


def solution(mesh):
    return jax.shard_map(
        shards,
        mesh=mesh,
        in_specs=(
            P(("cfg", "tm"), "space", None, None),
            P(("cfg", "tm"), None, None, "space"),
            P(),
            P(),
        ),
        out_specs=P("space", ("cfg", "tm"), None, None, None),
        check_vma=False,
    )
```

```python
import functools
import math

import jax
import jax.numpy as jnp
from jax import lax
from jax.experimental import pallas as pl
from jax.experimental.pallas import tpu as pltpu
from jax.sharding import PartitionSpec as P

LXY = 32
NMOM = 8
NDIR = 3
PLANE = LXY * LXY
LANES = 128
BLOCKS = PLANE // LANES
HALF = PLANE // 2
COMPS = 6
BLOCK_ROWS = COMPS * BLOCKS
PITCH = BLOCK_ROWS + 8
DEPTH = COMPS * PLANE
TWO_PI = 2.0 * math.pi
MESH = pl.DeviceIdType.MESH
BF16, F32 = jnp.bfloat16, jnp.float32


def roll(value, shift):
    return pltpu.roll(value, shift, value.ndim - 1)


def apply_table(table, lanes, field):
    out_re, out_im = [], []
    for row in range(3):
        acc_re = acc_im = None
        for col in range(3):
            link_re = table[3 * row + col : 3 * row + col + 1, lanes]
            link_im = table[9 + 3 * row + col : 10 + 3 * row + col, lanes]
            re = link_re * field[col] - link_im * field[3 + col]
            im = link_re * field[3 + col] + link_im * field[col]
            acc_re = re if acc_re is None else acc_re + re
            acc_im = im if acc_im is None else acc_im + im
        out_re.append(acc_re)
        out_im.append(acc_im)
    return out_re + out_im


def minus_adjoint(entries):
    real = [-entries[3 * b + a] for a in range(3) for b in range(3)]
    imag = [entries[9 + 3 * b + a] for a in range(3) for b in range(3)]
    return real + imag


def lanes_at(slot, at):
    return pl.ds(pl.multiple_of(slot * PLANE + at * LANES, LANES), LANES)


def store_packed(packed, base, first, nev, rows_at, group, at, value):
    for colour in range(3):
        re = value[colour].astype(BF16)
        im = value[3 + colour].astype(BF16)
        upper, lower = pl.ds(base + rows_at, group), pl.ds(base + nev + rows_at, group)
        packed[upper, lanes_at(first + colour, at)] = re
        packed[lower, lanes_at(first + colour, at)] = im
        packed[upper, lanes_at(first + 3 + colour, at)] = im
        packed[lower, lanes_at(first + 3 + colour, at)] = -re


def store_twisted(twisted, first, nev, rows_at, group, at, cosine, sine, field):
    for mom in range(NMOM):
        cos_row = cosine[mom : mom + 1, lanes_at(0, at)]
        sin_row = sine[mom : mom + 1, lanes_at(0, at)]
        rows = pl.ds(mom * nev + rows_at, group)
        for colour in range(3):
            vec_re, vec_im = field[colour], field[3 + colour]
            twisted[rows, lanes_at(first + colour, at)] = (
                vec_re * cos_row - vec_im * sin_row
            ).astype(BF16)
            twisted[rows, lanes_at(first + 3 + colour, at)] = (
                vec_re * sin_row + vec_im * cos_row
            ).astype(BF16)


def contract(left, right):
    return lax.dot_general(left, right, (((1,), (1,)), ((), ())), preferred_element_type=F32)


def wait_for(ref, sem):
    pltpu.make_async_copy(ref, ref, sem).wait()


def fill_phases(momenta, plane, z_length, cosine, sine):
    row = lax.broadcasted_iota(jnp.int32, (NMOM, LANES), 0)
    lane = lax.broadcasted_iota(jnp.int32, (NMOM, LANES), 1)

    def column(axis):
        value = jnp.zeros((NMOM, LANES), jnp.int32)
        for mom in range(NMOM):
            value = jnp.where(row == mom, momenta[axis, mom], value)
        return value

    mom_x, mom_y, mom_z = column(0), column(1), column(2)
    part_x = jnp.bitwise_and(mom_x * jnp.bitwise_and(lane, LXY - 1), LXY - 1).astype(F32) / LXY
    y_low = jnp.right_shift(lane, LXY.bit_length() - 1)
    for at in range(BLOCKS):
        y_coord = y_low + at * (LANES // LXY)
        part_y = jnp.bitwise_and(mom_y * y_coord, LXY - 1).astype(F32) / LXY
        beside = plane + 1 if at < BLOCKS // 2 else plane + z_length - 1
        for index, z_coord in enumerate((plane, beside)):
            part_z = jnp.bitwise_and(mom_z * z_coord, z_length - 1).astype(F32) / z_length
            theta = TWO_PI * (part_x + part_y + part_z)
            cosine[index, :, at * LANES : (at + 1) * LANES] = jnp.cos(theta)
            sine[index, :, at * LANES : (at + 1) * LANES] = jnp.sin(theta)


def pack_links(links_ref, links_out, links_z_out):
    for at in range(BLOCKS):
        lanes = slice(at * LANES, (at + 1) * LANES)
        rows = [links_ref[direction, :, lanes].astype(F32) for direction in range(NDIR)]
        for direction in range(NDIR):
            links_out[at, direction * 24 : direction * 24 + 18, :] = rows[direction].astype(BF16)
        if at >= BLOCKS // 2:
            links_z_out[at - BLOCKS // 2, 0:18, :] = rows[2].astype(BF16)


def fill_tables(links, table):
    lane = lax.broadcasted_iota(jnp.int32, (1, LANES), 1)
    x_lane = jnp.bitwise_and(lane, LXY - 1)

    def block(index):
        return slice(index * LANES, (index + 1) * LANES)

    for direction in range(2):
        for at in range(BLOCKS):
            wide = 0.5 * links[at, direction * 24 : direction * 24 + 24, :].astype(F32)
            own = [wide[e : e + 1] for e in range(18)]
            if direction == 0:
                moved = [jnp.where(x_lane == 0, roll(u, 97), roll(u, 1)) for u in own]
            else:
                before = (at + BLOCKS - 1) % BLOCKS
                wide = 0.5 * links[before, direction * 24 : direction * 24 + 24, :].astype(F32)
                other = [wide[e : e + 1] for e in range(18)]
                moved = [
                    jnp.where(lane < LXY, roll(o, LXY), roll(u, LXY)) for o, u in zip(other, own)
                ]
            for e in range(18):
                table[2 * direction, e : e + 1, block(at)] = own[e]
            for e, value in enumerate(minus_adjoint(moved)):
                table[2 * direction + 1, e : e + 1, block(at)] = value


def fill_z_tables(links, links_z, table):
    for at in range(BLOCKS):
        lanes = slice(at * LANES, (at + 1) * LANES)
        if at < BLOCKS // 2:
            wide = 0.5 * links[at, 48:72, :].astype(F32)
            straight, turned = 4, 5
        else:
            wide = 0.5 * links_z[at - BLOCKS // 2, 0:24, :].astype(F32)
            straight, turned = 5, 4
        own = [wide[e : e + 1] for e in range(18)]
        for e in range(18):
            table[straight, e : e + 1, lanes] = own[e]
        for e, value in enumerate(minus_adjoint(own)):
            table[turned, e : e + 1, lanes] = value


def fill_order(core, side, order):
    bits = side.bit_length() - 1
    width = 2 * side * side
    row = lax.broadcasted_iota(jnp.int32, (width, width), 0)
    column = lax.broadcasted_iota(jnp.int32, (width, width), 1)
    low = jnp.bitwise_and(row, side - 1)
    place = jnp.bitwise_and(jnp.right_shift(row, bits), side - 1)
    rest = row - low - place * side
    high = jnp.right_shift(place, 1) + (side // 2) * jnp.bitwise_and(place, 1)
    number = jnp.where(core == 1, low * side + high, high * side + low)
    order[...] = jnp.where(column == rest + number, 1.0, 0.0)


def kernel(
    side, x_ref, links_ref, momenta_ref, directions_ref, out_ref,
    ra, rb, spread, field, field_b, halo, links_z_out, links, links_z, table, cosine, sine, order,
    twisted, twisted_h, packed_xy, packed_z, packed_h, acc_xy, acc_z, send_xy, send_z, got_xy, got_z,
    sum_xy, sum_z, rows_out, rows_in, last,
    ready, sem_a, sem_b, sem_h, sem_l, sem_r, sem_s,
):
    nev = side * side
    pairs = side // 2
    group = 2 * side
    me, core = lax.axis_index("space"), lax.axis_index("tm")
    high, low = me // side, me % side
    a = low + core * (high - low)
    b = high + core * (low - high)

    def device(at_a, at_b):
        return (1 - core) * (at_b * side + at_a) + core * (at_a * side + at_b)

    above = (me + 1) % nev
    below = (me + nev - 1) % nev

    barrier = pltpu.get_barrier_semaphore()

    def greet(target):
        pl.semaphore_signal(barrier, inc=1, device_id={"space": target}, device_id_type=MESH)

    beside_b = (device(a, (b + 1) % side), device(a, (b + side - 1) % side))
    for step in range(1, side):
        greet(device((a + step) % side, b))
    for target in (above, below) + beside_b:
        greet(target)
    pack_links(links_ref, links, links_z_out)
    pl.semaphore_wait(barrier, side - 1 + 4)

    def send(src, dst, sent, arrived, target):
        copy = pltpu.make_async_remote_copy(
            src_ref=src, dst_ref=dst, send_sem=sent, recv_sem=arrived,
            device_id={"space": target}, device_id_type=MESH,
        )
        copy.start()
        return copy

    far_a = sorted(range(1, side), key=lambda k: -min(k, side - k))
    turns = [0] + sorted(range(1, pairs), key=lambda k: -min(k, pairs - k))

    def member_of(turn, member):
        return (b + turn) % pairs + member * pairs

    for step in far_a:
        to_a = (a + step) % side

        @pl.when(core == 0)
        def _():
            send(x_ref.at[:, to_a], ra.at[a], sem_s.at[2], sem_a, device(to_a, b))

        @pl.when(core == 1)
        def _():
            send(x_ref.at[to_a], ra.at[a], sem_s.at[2], sem_a, device(to_a, b))

    links_copy = send(links_z_out, links_z, sem_s.at[1], sem_l, above)
    for to_b in range(side):
        ra[a, to_b] = x_ref[
            (1 - core) * to_b + core * a, (1 - core) * a + core * to_b
        ]
    fill_phases(momenta_ref, me, nev, cosine, sine)
    fill_order(core, side, order)
    fill_tables(links, table)

    for place in range(side // 2 - 1):
        for target in beside_b:
            pl.semaphore_signal(
                ready.at[place], inc=1, device_id={"space": target}, device_id_type=MESH
            )
        pl.semaphore_wait(ready.at[place], 2)

    wait_for(ra.at[pl.ds(0, side - 1)], sem_a)
    for turn in turns:
        for member in range(2 if turn else 1):
            to_b = member_of(turn, member) if turn else (b + pairs) % side
            send(ra.at[:, to_b], rb.at[b], sem_s.at[3], sem_b.at[turn], device(a, to_b))
    for from_a in range(side):
        rb[b, from_a] = ra[from_a, b]

    links_copy.wait()
    fill_z_tables(links, links_z, table)
    upper = pl.ds(HALF, HALF)
    lane = lax.broadcasted_iota(jnp.int32, (1, LANES), 1)
    x_lane = jnp.bitwise_and(lane, LXY - 1)
    lower_half = pl.ds(0, HALF)

    def pair_of(turn):
        return (b + pairs - turn) % pairs

    def own_plane(turn):
        pair = pair_of(turn)
        rows_at = pl.multiple_of(pair * group, group)
        wait_for(rb.at[pl.ds(0, 2 if turn else 1)], sem_b.at[turn])
        for member in range(2):
            for from_a in range(side):
                spread[pl.ds((member * side + from_a) * PITCH, BLOCK_ROWS), :] = rb[
                    pair + member * pairs, from_a
                ].astype(F32)
        for comp in range(COMPS):
            for at in range(BLOCKS):
                rows = spread[pl.ds(comp * BLOCKS + at, group, stride=PITCH), :]
                field[comp, :, at * LANES : (at + 1) * LANES] = rows
                field_b[pair, comp, :, at * LANES : (at + 1) * LANES] = rows.astype(BF16)
        send(
            field_b.at[pair, :, :, lower_half], halo.at[pair, :, :, lower_half],
            sem_s.at[4], sem_h.at[0, pair], below,
        )
        send(
            field_b.at[pair, :, :, upper], halo.at[pair, :, :, upper],
            sem_s.at[4], sem_h.at[1, pair], above,
        )

        @pl.loop(0, BLOCKS)
        def _(at):
            lanes = lanes_at(0, at)
            after = lanes_at(0, (at + 1) % BLOCKS)
            before = lanes_at(0, (at + BLOCKS - 1) % BLOCKS)
            vec = [field[c, :, lanes] for c in range(COMPS)]
            store_twisted(twisted, 0, nev, rows_at, group, at, cosine.at[0], sine.at[0], vec)
            ahead = [jnp.where(x_lane == LXY - 1, roll(v, 31), roll(v, 127)) for v in vec]
            behind = [jnp.where(x_lane == 0, roll(v, 97), roll(v, 1)) for v in vec]
            first = apply_table(table.at[0], lanes, ahead)
            second = apply_table(table.at[1], lanes, behind)
            store_packed(
                packed_xy, 0, 0, nev, rows_at, group, at, [f + s for f, s in zip(first, second)]
            )
            ahead = [
                jnp.where(lane < LANES - LXY, roll(v, 96), roll(field[c, :, after], 96))
                for c, v in enumerate(vec)
            ]
            behind = [
                jnp.where(lane < LXY, roll(field[c, :, before], LXY), roll(v, LXY))
                for c, v in enumerate(vec)
            ]
            first = apply_table(table.at[2], lanes, ahead)
            second = apply_table(table.at[3], lanes, behind)
            store_packed(
                packed_xy, 2 * nev, 0, nev, rows_at, group, at,
                [f + s for f, s in zip(first, second)],
            )
            store_packed(
                packed_h, 0, 0, nev, rows_at, group, at,
                apply_table(table.at[5], lanes, vec),
            )

    def halo_wait(which):
        for turn in which:
            wait_for(halo.at[0, :, :, lower_half], sem_h.at[0, pair_of(turn)])
            wait_for(halo.at[0, :, :, upper], sem_h.at[1, pair_of(turn)])

    def beside_block(turn, at):
        pair = pair_of(turn)
        rows_at = pl.multiple_of(pair * group, group)
        lanes = lanes_at(0, at)
        vec = [halo[pair, c, :, lanes].astype(F32) for c in range(COMPS)]
        store_twisted(twisted_h, 0, nev, rows_at, group, at, cosine.at[1], sine.at[1], vec)
        store_packed(
            packed_z, 0, 0, nev, rows_at, group, at, apply_table(table.at[4], lanes, vec)
        )

    def spread_sums(acc, parts, outgoing, got, sent, sem):
        width = parts * side
        for to_a in range(side):
            for mom in range(NMOM):
                for index in range(parts):
                    at = mom * width + index * side
                    outgoing[to_a, at : at + side, :] = acc[
                        index, pl.ds(mom * nev + to_a, side, stride=side), :
                    ].astype(BF16)
        for step in far_a:
            to_a = (a + step) % side
            send(outgoing.at[to_a], got.at[step - 1], sent, sem, device(to_a, b))

    def collect_sums(outgoing, got, total, sem):
        wait_for(got, sem)
        value = outgoing[a].astype(F32)
        for index in range(side - 1):
            value = value + got[index].astype(F32)
        total[...] = value

    for turn in turns:
        own_plane(turn)
    halo_wait(turns[:-1])
    acc_xy[...] = jnp.zeros_like(acc_xy)

    @pl.loop(0, BLOCKS // 2)
    def _(half):
        total = None
        for slot in range(COMPS):
            part = pl.ds(pl.multiple_of(slot * PLANE + half * 2 * LANES, 2 * LANES), 2 * LANES)
            product = contract(twisted[:, part], packed_xy[:, part])
            total = product if total is None else total + product
        for index in range(2):
            acc_xy[index] += total[:, index * 2 * nev : (index + 1) * 2 * nev]
        for turn in turns[:-1]:
            for at in range(2):
                beside_block(turn, 2 * half + at)

    spread_sums(acc_xy, 2, send_xy, got_xy, sem_s.at[5], sem_r.at[0])
    halo_wait(turns[-1:])

    @pl.loop(0, BLOCKS)
    def _(at):
        beside_block(turns[-1], at)

    acc_z[0] = contract(twisted[...], packed_z[...]) + contract(twisted_h[...], packed_h[...])
    spread_sums(acc_z, 1, send_z, got_z, sem_s.at[6], sem_r.at[1])

    collect_sums(send_xy, got_xy, sum_xy, sem_r.at[0])
    collect_sums(send_z, got_z, sum_z, sem_r.at[1])
    for place in range(side):
        rows_out[place, 0 : 2 * NMOM, :] = sum_xy[pl.ds(place, 2 * NMOM, stride=side), :]
        rows_out[place, 2 * NMOM :, :] = sum_z[pl.ds(place, NMOM, stride=side), :]

    def place_of(at_b):
        return 2 * (at_b % pairs) + at_b // pairs

    for step in far_a:
        to_b = (b + step) % side
        send(rows_out.at[place_of(to_b)], rows_in.at[step - 1], sem_s.at[7], sem_r.at[2], device(a, to_b))
    wait_for(rows_in, sem_r.at[2])
    value = rows_out[place_of(b)]
    for index in range(side - 1):
        value = value + rows_in[index]
    last[...] = jnp.dot(
        value, order[...], preferred_element_type=F32, precision=lax.Precision.HIGHEST
    )
    by_dir = [
        last[pl.ds(0, NMOM, stride=2), :],
        last[pl.ds(1, NMOM, stride=2), :],
        last[2 * NMOM :, :],
    ]
    for slot in range(NDIR):
        chosen = directions_ref[slot]
        out_ref[slot] = jnp.where(
            chosen == 0, by_dir[0], jnp.where(chosen == 1, by_dir[1], by_dir[2])
        )

    wait_for(ra.at[pl.ds(0, side - 1)], sem_s.at[2])
    wait_for(rb.at[pl.ds(0, side - 1)], sem_s.at[3])
    wait_for(field_b, sem_s.at[4])
    wait_for(got_xy, sem_s.at[5])
    wait_for(got_z, sem_s.at[6])
    wait_for(rows_in, sem_s.at[7])


def shards(vectors, gauge_links, momenta, directions):
    space = lax.axis_size("space")
    side = math.isqrt(space)
    nev, pairs, group = space, side // 2, 2 * side
    blocks = vectors.reshape(COMPS, space, BLOCKS, LANES)
    blocks = jnp.transpose(blocks, (1, 0, 2, 3)).reshape(side, side, BLOCK_ROWS, LANES)
    scratch = [
        ((side, side, BLOCK_ROWS, LANES), BF16),
        ((side, side, BLOCK_ROWS, LANES), BF16),
        ((group * PITCH, LANES), F32),
        ((COMPS, group, PLANE), F32),
        ((pairs, COMPS, group, PLANE), BF16),
        ((pairs, COMPS, group, PLANE), BF16),
        ((BLOCKS // 2, 32, LANES), BF16),
        ((BLOCKS, 80, LANES), BF16),
        ((BLOCKS // 2, 32, LANES), BF16),
        ((6, 24, PLANE), F32),
        ((2, NMOM, PLANE), F32),
        ((2, NMOM, PLANE), F32),
        ((2 * nev, 2 * nev), F32),
        ((NMOM * nev, DEPTH), BF16),
        ((NMOM * nev, DEPTH), BF16),
        ((4 * nev, DEPTH), BF16),
        ((2 * nev, DEPTH), BF16),
        ((2 * nev, DEPTH), BF16),
        ((2, NMOM * nev, 2 * nev), F32),
        ((1, NMOM * nev, 2 * nev), F32),
        ((side, 2 * NMOM * side, 2 * nev), BF16),
        ((side, NMOM * side, 2 * nev), BF16),
        ((side - 1, 2 * NMOM * side, 2 * nev), BF16),
        ((side - 1, NMOM * side, 2 * nev), BF16),
        ((2 * NMOM * side, 2 * nev), F32),
        ((NMOM * side, 2 * nev), F32),
        ((side, NDIR * NMOM, 2 * nev), F32),
        ((side - 1, NDIR * NMOM, 2 * nev), F32),
        ((NDIR * NMOM, 2 * nev), F32),
    ]
    dma = pltpu.SemaphoreType.DMA
    out = pl.pallas_call(
        functools.partial(kernel, side),
        out_shape=jax.ShapeDtypeStruct((NDIR, NMOM, 2 * nev), F32),
        in_specs=[
            pl.BlockSpec(memory_space=pltpu.VMEM),
            pl.BlockSpec(memory_space=pltpu.VMEM),
            pl.BlockSpec(memory_space=pltpu.SMEM),
            pl.BlockSpec(memory_space=pltpu.SMEM),
        ],
        out_specs=pl.BlockSpec(memory_space=pltpu.VMEM),
        scratch_shapes=[pltpu.VMEM(*s) for s in scratch]
        + [pltpu.SemaphoreType.REGULAR((max(1, side // 2 - 1),))]
        + [dma, dma((pairs,)), dma((2, pairs)), dma, dma((3,)), dma((8,))],
        compiler_params=pltpu.CompilerParams(
            collective_id=0, has_side_effects=True, vmem_limit_bytes=60 * 1024 * 1024
        ),
    )(blocks, gauge_links[0], momenta.T, directions)
    return jnp.transpose(out, (1, 0, 2))[None, None]


def solution(mesh):
    return jax.shard_map(
        shards,
        mesh=mesh,
        in_specs=(
            P(("cfg", "tm"), "space", None, None),
            P(("cfg", "tm"), None, None, "space"),
            P(),
            P(),
        ),
        out_specs=P("space", ("cfg", "tm"), None, None, None),
        check_vma=False,
    )
```

```python
import functools
import math

import jax
import jax.numpy as jnp
from jax import lax
from jax.experimental import pallas as pl
from jax.experimental.pallas import tpu as pltpu
from jax.sharding import PartitionSpec as P

LXY = 32
NMOM = 8
NDIR = 3
PLANE = LXY * LXY
LANES = 128
BLOCKS = PLANE // LANES
HALF = PLANE // 2
COMPS = 6
BLOCK_ROWS = COMPS * BLOCKS
PITCH = BLOCK_ROWS + 8
DEPTH = COMPS * PLANE
TWO_PI = 2.0 * math.pi
MESH = pl.DeviceIdType.MESH
BF16, F32 = jnp.bfloat16, jnp.float32


def roll(value, shift):
    return pltpu.roll(value, shift, value.ndim - 1)


def apply_table(table, lanes, field):
    out_re, out_im = [], []
    for row in range(3):
        acc_re = acc_im = None
        for col in range(3):
            link_re = table[3 * row + col : 3 * row + col + 1, lanes]
            link_im = table[9 + 3 * row + col : 10 + 3 * row + col, lanes]
            re = link_re * field[col] - link_im * field[3 + col]
            im = link_re * field[3 + col] + link_im * field[col]
            acc_re = re if acc_re is None else acc_re + re
            acc_im = im if acc_im is None else acc_im + im
        out_re.append(acc_re)
        out_im.append(acc_im)
    return out_re + out_im


def minus_adjoint(entries):
    real = [-entries[3 * b + a] for a in range(3) for b in range(3)]
    imag = [entries[9 + 3 * b + a] for a in range(3) for b in range(3)]
    return real + imag


def lanes_at(slot, at):
    return pl.ds(pl.multiple_of(slot * PLANE + at * LANES, LANES), LANES)


def store_packed(packed, base, first, nev, rows_at, group, at, value):
    for colour in range(3):
        re = value[colour].astype(BF16)
        im = value[3 + colour].astype(BF16)
        upper, lower = pl.ds(base + rows_at, group), pl.ds(base + nev + rows_at, group)
        packed[upper, lanes_at(first + colour, at)] = re
        packed[lower, lanes_at(first + colour, at)] = im
        packed[upper, lanes_at(first + 3 + colour, at)] = im
        packed[lower, lanes_at(first + 3 + colour, at)] = -re


def store_twisted(twisted, first, nev, rows_at, group, at, cosine, sine, field):
    for mom in range(NMOM):
        cos_row = cosine[mom : mom + 1, lanes_at(0, at)]
        sin_row = sine[mom : mom + 1, lanes_at(0, at)]
        rows = pl.ds(mom * nev + rows_at, group)
        for colour in range(3):
            vec_re, vec_im = field[colour], field[3 + colour]
            twisted[rows, lanes_at(first + colour, at)] = (
                vec_re * cos_row - vec_im * sin_row
            ).astype(BF16)
            twisted[rows, lanes_at(first + 3 + colour, at)] = (
                vec_re * sin_row + vec_im * cos_row
            ).astype(BF16)


def contract(left, right):
    return lax.dot_general(left, right, (((1,), (1,)), ((), ())), preferred_element_type=F32)


def wait_for(ref, sem):
    pltpu.make_async_copy(ref, ref, sem).wait()


def fill_phases(momenta, plane, z_length, cosine, sine):
    row = lax.broadcasted_iota(jnp.int32, (NMOM, LANES), 0)
    lane = lax.broadcasted_iota(jnp.int32, (NMOM, LANES), 1)

    def column(axis):
        value = jnp.zeros((NMOM, LANES), jnp.int32)
        for mom in range(NMOM):
            value = jnp.where(row == mom, momenta[axis, mom], value)
        return value

    mom_x, mom_y, mom_z = column(0), column(1), column(2)
    part_x = jnp.bitwise_and(mom_x * jnp.bitwise_and(lane, LXY - 1), LXY - 1).astype(F32) / LXY
    y_low = jnp.right_shift(lane, LXY.bit_length() - 1)
    for at in range(BLOCKS):
        y_coord = y_low + at * (LANES // LXY)
        part_y = jnp.bitwise_and(mom_y * y_coord, LXY - 1).astype(F32) / LXY
        beside = plane + 1 if at < BLOCKS // 2 else plane + z_length - 1
        for index, z_coord in enumerate((plane, beside)):
            part_z = jnp.bitwise_and(mom_z * z_coord, z_length - 1).astype(F32) / z_length
            theta = TWO_PI * (part_x + part_y + part_z)
            cosine[index, :, at * LANES : (at + 1) * LANES] = jnp.cos(theta)
            sine[index, :, at * LANES : (at + 1) * LANES] = jnp.sin(theta)


def pack_links(links_ref, links_out, links_z_out):
    for at in range(BLOCKS):
        lanes = slice(at * LANES, (at + 1) * LANES)
        rows = [links_ref[direction, :, lanes].astype(F32) for direction in range(NDIR)]
        for direction in range(NDIR):
            links_out[at, direction * 24 : direction * 24 + 18, :] = rows[direction].astype(BF16)
        if at >= BLOCKS // 2:
            links_z_out[at - BLOCKS // 2, 0:18, :] = rows[2].astype(BF16)


def fill_tables(links, table):
    lane = lax.broadcasted_iota(jnp.int32, (1, LANES), 1)
    x_lane = jnp.bitwise_and(lane, LXY - 1)

    def block(index):
        return slice(index * LANES, (index + 1) * LANES)

    for direction in range(2):
        for at in range(BLOCKS):
            wide = 0.5 * links[at, direction * 24 : direction * 24 + 24, :].astype(F32)
            own = [wide[e : e + 1] for e in range(18)]
            if direction == 0:
                moved = [jnp.where(x_lane == 0, roll(u, 97), roll(u, 1)) for u in own]
            else:
                before = (at + BLOCKS - 1) % BLOCKS
                wide = 0.5 * links[before, direction * 24 : direction * 24 + 24, :].astype(F32)
                other = [wide[e : e + 1] for e in range(18)]
                moved = [
                    jnp.where(lane < LXY, roll(o, LXY), roll(u, LXY)) for o, u in zip(other, own)
                ]
            for e in range(18):
                table[2 * direction, e : e + 1, block(at)] = own[e]
            for e, value in enumerate(minus_adjoint(moved)):
                table[2 * direction + 1, e : e + 1, block(at)] = value


def fill_z_tables(links, links_z, table):
    for at in range(BLOCKS):
        lanes = slice(at * LANES, (at + 1) * LANES)
        if at < BLOCKS // 2:
            wide = 0.5 * links[at, 48:72, :].astype(F32)
            straight, turned = 4, 5
        else:
            wide = 0.5 * links_z[at - BLOCKS // 2, 0:24, :].astype(F32)
            straight, turned = 5, 4
        own = [wide[e : e + 1] for e in range(18)]
        for e in range(18):
            table[straight, e : e + 1, lanes] = own[e]
        for e, value in enumerate(minus_adjoint(own)):
            table[turned, e : e + 1, lanes] = value


def fill_order(core, side, order):
    bits = side.bit_length() - 1
    width = 2 * side * side
    row = lax.broadcasted_iota(jnp.int32, (width, width), 0)
    column = lax.broadcasted_iota(jnp.int32, (width, width), 1)
    low = jnp.bitwise_and(row, side - 1)
    place = jnp.bitwise_and(jnp.right_shift(row, bits), side - 1)
    rest = row - low - place * side
    high = jnp.right_shift(place, 1) + (side // 2) * jnp.bitwise_and(place, 1)
    number = jnp.where(core == 1, low * side + high, high * side + low)
    order[...] = jnp.where(column == rest + number, 1.0, 0.0)


def kernel(
    side, x_ref, links_ref, momenta_ref, directions_ref, out_ref,
    ra, rb, spread, field, field_b, halo, links_z_out, links, links_z, table, cosine, sine, order,
    twisted, twisted_h, packed_xy, packed_z, packed_h, acc_xy, acc_z, send_xy, send_z, got_xy, got_z,
    sum_xy, sum_z, rows_out, rows_in, last,
    ready, sem_a, sem_b, sem_h, sem_l, sem_r, sem_s,
):
    nev = side * side
    pairs = side // 2
    group = 2 * side
    me, core = lax.axis_index("space"), lax.axis_index("tm")
    high, low = me // side, me % side
    a = low + core * (high - low)
    b = high + core * (low - high)

    def device(at_a, at_b):
        return (1 - core) * (at_b * side + at_a) + core * (at_a * side + at_b)

    above = (me + 1) % nev
    below = (me + nev - 1) % nev

    barrier = pltpu.get_barrier_semaphore()

    def greet(target):
        pl.semaphore_signal(barrier, inc=1, device_id={"space": target}, device_id_type=MESH)

    beside_b = (device(a, (b + 1) % side), device(a, (b + side - 1) % side))
    for step in range(1, side):
        greet(device((a + step) % side, b))
    for target in (above, below) + beside_b:
        greet(target)
    pack_links(links_ref, links, links_z_out)
    pl.semaphore_wait(barrier, side - 1 + 4)

    def send(src, dst, sent, arrived, target):
        copy = pltpu.make_async_remote_copy(
            src_ref=src, dst_ref=dst, send_sem=sent, recv_sem=arrived,
            device_id={"space": target}, device_id_type=MESH,
        )
        copy.start()
        return copy

    far_a = sorted(range(1, side), key=lambda k: -min(k, side - k))
    own_pair = b % pairs

    for step in far_a:
        to_a = (a + step) % side

        @pl.when(core == 0)
        def _():
            send(x_ref.at[:, to_a], ra.at[a], sem_s.at[2], sem_a, device(to_a, b))

        @pl.when(core == 1)
        def _():
            send(x_ref.at[to_a], ra.at[a], sem_s.at[2], sem_a, device(to_a, b))

    links_copy = send(links_z_out, links_z, sem_s.at[1], sem_l, above)
    for to_b in range(side):
        ra[a, to_b] = x_ref[
            (1 - core) * to_b + core * a, (1 - core) * a + core * to_b
        ]
    fill_phases(momenta_ref, me, nev, cosine, sine)
    fill_order(core, side, order)
    fill_tables(links, table)

    for place in range(side // 2 - 1):
        for target in beside_b:
            pl.semaphore_signal(
                ready.at[place], inc=1, device_id={"space": target}, device_id_type=MESH
            )
        pl.semaphore_wait(ready.at[place], 2)

    wait_for(ra.at[pl.ds(0, side - 1)], sem_a)
    for turn in reversed(range(pairs)):
        for member in range(2 if turn else 1):
            to_b = (b + turn) % pairs + member * pairs if turn else (b + pairs) % side
            send(ra.at[:, to_b], rb.at[b], sem_s.at[3], sem_b.at[own_pair], device(a, to_b))
    for from_a in range(side):
        rb[b, from_a] = ra[from_a, b]

    links_copy.wait()
    fill_z_tables(links, links_z, table)
    upper = pl.ds(HALF, HALF)
    lane = lax.broadcasted_iota(jnp.int32, (1, LANES), 1)
    x_lane = jnp.bitwise_and(lane, LXY - 1)
    lower_half = pl.ds(0, HALF)

    def own_plane(pair):
        rows_at = pl.multiple_of(pair * group, group)
        @pl.when(pair == own_pair)
        def _():
            wait_for(rb.at[pl.ds(0, 1)], sem_b.at[pair])

        @pl.when(pair != own_pair)
        def _():
            wait_for(rb.at[pl.ds(0, 2)], sem_b.at[pair])

        for member in range(2):
            for from_a in range(side):
                spread[pl.ds((member * side + from_a) * PITCH, BLOCK_ROWS), :] = rb[
                    pair + member * pairs, from_a
                ].astype(F32)
        for comp in range(COMPS):
            for at in range(BLOCKS):
                rows = spread[pl.ds(comp * BLOCKS + at, group, stride=PITCH), :]
                field[comp, :, at * LANES : (at + 1) * LANES] = rows
                field_b[pair, comp, :, at * LANES : (at + 1) * LANES] = rows.astype(BF16)
        send(
            field_b.at[pair, :, :, lower_half], halo.at[pair, :, :, lower_half],
            sem_s.at[4], sem_h.at[0, pair], below,
        )
        send(
            field_b.at[pair, :, :, upper], halo.at[pair, :, :, upper],
            sem_s.at[4], sem_h.at[1, pair], above,
        )

        @pl.loop(0, BLOCKS)
        def _(at):
            lanes = lanes_at(0, at)
            after = lanes_at(0, (at + 1) % BLOCKS)
            before = lanes_at(0, (at + BLOCKS - 1) % BLOCKS)
            vec = [field[c, :, lanes] for c in range(COMPS)]
            store_twisted(twisted, 0, nev, rows_at, group, at, cosine.at[0], sine.at[0], vec)
            ahead = [jnp.where(x_lane == LXY - 1, roll(v, 31), roll(v, 127)) for v in vec]
            behind = [jnp.where(x_lane == 0, roll(v, 97), roll(v, 1)) for v in vec]
            first = apply_table(table.at[0], lanes, ahead)
            second = apply_table(table.at[1], lanes, behind)
            store_packed(
                packed_xy, 0, 0, nev, rows_at, group, at, [f + s for f, s in zip(first, second)]
            )
            ahead = [
                jnp.where(lane < LANES - LXY, roll(v, 96), roll(field[c, :, after], 96))
                for c, v in enumerate(vec)
            ]
            behind = [
                jnp.where(lane < LXY, roll(field[c, :, before], LXY), roll(v, LXY))
                for c, v in enumerate(vec)
            ]
            first = apply_table(table.at[2], lanes, ahead)
            second = apply_table(table.at[3], lanes, behind)
            store_packed(
                packed_xy, 2 * nev, 0, nev, rows_at, group, at,
                [f + s for f, s in zip(first, second)],
            )
            store_packed(
                packed_h, 0, 0, nev, rows_at, group, at,
                apply_table(table.at[5], lanes, vec),
            )

    def halo_wait(which):
        for pair in which:
            wait_for(halo.at[0, :, :, lower_half], sem_h.at[0, pair])
            wait_for(halo.at[0, :, :, upper], sem_h.at[1, pair])

    def beside_block(pair, at):
        rows_at = pair * group
        lanes = lanes_at(0, at)
        vec = [halo[pair, c, :, lanes].astype(F32) for c in range(COMPS)]
        store_twisted(twisted_h, 0, nev, rows_at, group, at, cosine.at[1], sine.at[1], vec)
        store_packed(
            packed_z, 0, 0, nev, rows_at, group, at, apply_table(table.at[4], lanes, vec)
        )

    def spread_sums(acc, parts, outgoing, got, sent, sem):
        width = parts * side
        for to_a in range(side):
            for mom in range(NMOM):
                for index in range(parts):
                    at = mom * width + index * side
                    outgoing[to_a, at : at + side, :] = acc[
                        index, pl.ds(mom * nev + to_a, side, stride=side), :
                    ].astype(BF16)
        for step in far_a:
            to_a = (a + step) % side
            send(outgoing.at[to_a], got.at[step - 1], sent, sem, device(to_a, b))

    def collect_sums(outgoing, got, total, sem):
        wait_for(got, sem)
        value = outgoing[a].astype(F32)
        for index in range(side - 1):
            value = value + got[index].astype(F32)
        total[...] = value

    for index in range(pairs - 1):
        own_plane(1 + (index + own_pair) % (pairs - 1))
    own_plane(0)
    halo_wait(range(1, pairs))
    acc_xy[...] = jnp.zeros_like(acc_xy)

    @pl.loop(0, BLOCKS // 2)
    def _(half):
        total = None
        for slot in range(COMPS):
            part = pl.ds(pl.multiple_of(slot * PLANE + half * 2 * LANES, 2 * LANES), 2 * LANES)
            product = contract(twisted[:, part], packed_xy[:, part])
            total = product if total is None else total + product
        for index in range(2):
            acc_xy[index] += total[:, index * 2 * nev : (index + 1) * 2 * nev]
        for pair in range(1, pairs):
            for at in range(2):
                beside_block(pair, 2 * half + at)

    spread_sums(acc_xy, 2, send_xy, got_xy, sem_s.at[5], sem_r.at[0])
    halo_wait([0])

    @pl.loop(0, BLOCKS)
    def _(at):
        beside_block(0, at)

    acc_z[0] = contract(twisted[...], packed_z[...]) + contract(twisted_h[...], packed_h[...])
    spread_sums(acc_z, 1, send_z, got_z, sem_s.at[6], sem_r.at[1])

    collect_sums(send_xy, got_xy, sum_xy, sem_r.at[0])
    collect_sums(send_z, got_z, sum_z, sem_r.at[1])
    for place in range(side):
        rows_out[place, 0 : 2 * NMOM, :] = sum_xy[pl.ds(place, 2 * NMOM, stride=side), :]
        rows_out[place, 2 * NMOM :, :] = sum_z[pl.ds(place, NMOM, stride=side), :]

    def place_of(at_b):
        return 2 * (at_b % pairs) + at_b // pairs

    for step in far_a:
        to_b = (b + step) % side
        send(rows_out.at[place_of(to_b)], rows_in.at[step - 1], sem_s.at[7], sem_r.at[2], device(a, to_b))
    wait_for(rows_in, sem_r.at[2])
    value = rows_out[place_of(b)]
    for index in range(side - 1):
        value = value + rows_in[index]
    last[...] = jnp.dot(
        value, order[...], preferred_element_type=F32, precision=lax.Precision.HIGHEST
    )
    by_dir = [
        last[pl.ds(0, NMOM, stride=2), :],
        last[pl.ds(1, NMOM, stride=2), :],
        last[2 * NMOM :, :],
    ]
    for slot in range(NDIR):
        chosen = directions_ref[slot]
        out_ref[slot] = jnp.where(
            chosen == 0, by_dir[0], jnp.where(chosen == 1, by_dir[1], by_dir[2])
        )

    wait_for(ra.at[pl.ds(0, side - 1)], sem_s.at[2])
    wait_for(rb.at[pl.ds(0, side - 1)], sem_s.at[3])
    wait_for(field_b, sem_s.at[4])
    wait_for(got_xy, sem_s.at[5])
    wait_for(got_z, sem_s.at[6])
    wait_for(rows_in, sem_s.at[7])


def shards(vectors, gauge_links, momenta, directions):
    space = lax.axis_size("space")
    side = math.isqrt(space)
    nev, pairs, group = space, side // 2, 2 * side
    blocks = vectors.reshape(COMPS, space, BLOCKS, LANES)
    blocks = jnp.transpose(blocks, (1, 0, 2, 3)).reshape(side, side, BLOCK_ROWS, LANES)
    scratch = [
        ((side, side, BLOCK_ROWS, LANES), BF16),
        ((side, side, BLOCK_ROWS, LANES), BF16),
        ((group * PITCH, LANES), F32),
        ((COMPS, group, PLANE), F32),
        ((pairs, COMPS, group, PLANE), BF16),
        ((pairs, COMPS, group, PLANE), BF16),
        ((BLOCKS // 2, 32, LANES), BF16),
        ((BLOCKS, 80, LANES), BF16),
        ((BLOCKS // 2, 32, LANES), BF16),
        ((6, 24, PLANE), F32),
        ((2, NMOM, PLANE), F32),
        ((2, NMOM, PLANE), F32),
        ((2 * nev, 2 * nev), F32),
        ((NMOM * nev, DEPTH), BF16),
        ((NMOM * nev, DEPTH), BF16),
        ((4 * nev, DEPTH), BF16),
        ((2 * nev, DEPTH), BF16),
        ((2 * nev, DEPTH), BF16),
        ((2, NMOM * nev, 2 * nev), F32),
        ((1, NMOM * nev, 2 * nev), F32),
        ((side, 2 * NMOM * side, 2 * nev), BF16),
        ((side, NMOM * side, 2 * nev), BF16),
        ((side - 1, 2 * NMOM * side, 2 * nev), BF16),
        ((side - 1, NMOM * side, 2 * nev), BF16),
        ((2 * NMOM * side, 2 * nev), F32),
        ((NMOM * side, 2 * nev), F32),
        ((side, NDIR * NMOM, 2 * nev), F32),
        ((side - 1, NDIR * NMOM, 2 * nev), F32),
        ((NDIR * NMOM, 2 * nev), F32),
    ]
    dma = pltpu.SemaphoreType.DMA
    out = pl.pallas_call(
        functools.partial(kernel, side),
        out_shape=jax.ShapeDtypeStruct((NDIR, NMOM, 2 * nev), F32),
        in_specs=[
            pl.BlockSpec(memory_space=pltpu.VMEM),
            pl.BlockSpec(memory_space=pltpu.VMEM),
            pl.BlockSpec(memory_space=pltpu.SMEM),
            pl.BlockSpec(memory_space=pltpu.SMEM),
        ],
        out_specs=pl.BlockSpec(memory_space=pltpu.VMEM),
        scratch_shapes=[pltpu.VMEM(*s) for s in scratch]
        + [pltpu.SemaphoreType.REGULAR((max(1, side // 2 - 1),))]
        + [dma, dma((pairs,)), dma((2, pairs)), dma, dma((3,)), dma((8,))],
        compiler_params=pltpu.CompilerParams(
            collective_id=0, has_side_effects=True, vmem_limit_bytes=60 * 1024 * 1024
        ),
    )(blocks, gauge_links[0], momenta.T, directions)
    return jnp.transpose(out, (1, 0, 2))[None, None]


def solution(mesh):
    return jax.shard_map(
        shards,
        mesh=mesh,
        in_specs=(
            P(("cfg", "tm"), "space", None, None),
            P(("cfg", "tm"), None, None, "space"),
            P(),
            P(),
        ),
        out_specs=P("space", ("cfg", "tm"), None, None, None),
        check_vma=False,
    )
```

```python
import functools
import math

import jax
import jax.numpy as jnp
from jax import lax
from jax.experimental import pallas as pl
from jax.experimental.pallas import tpu as pltpu
from jax.sharding import PartitionSpec as P

LXY = 32
NMOM = 8
NDIR = 3
PLANE = LXY * LXY
LANES = 128
BLOCKS = PLANE // LANES
HALF = PLANE // 2
COMPS = 6
BLOCK_ROWS = COMPS * BLOCKS
PITCH = BLOCK_ROWS + 8
DEPTH = COMPS * PLANE
TWO_PI = 2.0 * math.pi
MESH = pl.DeviceIdType.MESH
BF16, F32 = jnp.bfloat16, jnp.float32


def roll(value, shift):
    return pltpu.roll(value, shift, value.ndim - 1)


def apply_table(table, lanes, field):
    out_re, out_im = [], []
    for row in range(3):
        acc_re = acc_im = None
        for col in range(3):
            link_re = table[3 * row + col : 3 * row + col + 1, lanes]
            link_im = table[9 + 3 * row + col : 10 + 3 * row + col, lanes]
            re = link_re * field[col] - link_im * field[3 + col]
            im = link_re * field[3 + col] + link_im * field[col]
            acc_re = re if acc_re is None else acc_re + re
            acc_im = im if acc_im is None else acc_im + im
        out_re.append(acc_re)
        out_im.append(acc_im)
    return out_re + out_im


def minus_adjoint(entries):
    real = [-entries[3 * b + a] for a in range(3) for b in range(3)]
    imag = [entries[9 + 3 * b + a] for a in range(3) for b in range(3)]
    return real + imag


def lanes_at(slot, at):
    return pl.ds(pl.multiple_of(slot * PLANE + at * LANES, LANES), LANES)


def store_packed(packed, base, first, nev, rows_at, group, at, value):
    for colour in range(3):
        re = value[colour].astype(BF16)
        im = value[3 + colour].astype(BF16)
        upper, lower = pl.ds(base + rows_at, group), pl.ds(base + nev + rows_at, group)
        packed[upper, lanes_at(first + colour, at)] = re
        packed[lower, lanes_at(first + colour, at)] = im
        packed[upper, lanes_at(first + 3 + colour, at)] = im
        packed[lower, lanes_at(first + 3 + colour, at)] = -re


def store_twisted(twisted, pair, group, at, cosine, sine, field):
    for mom in range(NMOM):
        cos_row = cosine[mom : mom + 1, lanes_at(0, at)]
        sin_row = sine[mom : mom + 1, lanes_at(0, at)]
        rows = pl.ds(pl.multiple_of(pair * NMOM * group, group) + mom * group, group)
        for colour in range(3):
            vec_re, vec_im = field[colour], field[3 + colour]
            twisted[rows, lanes_at(colour, at)] = (
                vec_re * cos_row - vec_im * sin_row
            ).astype(BF16)
            twisted[rows, lanes_at(3 + colour, at)] = (
                vec_re * sin_row + vec_im * cos_row
            ).astype(BF16)


def contract(left, right):
    return lax.dot_general(left, right, (((1,), (1,)), ((), ())), preferred_element_type=F32)


def rounds_of(side):
    return (side - 1).bit_length() if side > 2 else 0


def wait_for(ref, sem):
    pltpu.make_async_copy(ref, ref, sem).wait()


def fill_phases(momenta, plane, z_length, cosine, sine):
    row = lax.broadcasted_iota(jnp.int32, (NMOM, LANES), 0)
    lane = lax.broadcasted_iota(jnp.int32, (NMOM, LANES), 1)

    def column(axis):
        value = jnp.zeros((NMOM, LANES), jnp.int32)
        for mom in range(NMOM):
            value = jnp.where(row == mom, momenta[axis, mom], value)
        return value

    mom_x, mom_y, mom_z = column(0), column(1), column(2)
    part_x = jnp.bitwise_and(mom_x * jnp.bitwise_and(lane, LXY - 1), LXY - 1).astype(F32) / LXY
    y_low = jnp.right_shift(lane, LXY.bit_length() - 1)
    for at in range(BLOCKS):
        y_coord = y_low + at * (LANES // LXY)
        part_y = jnp.bitwise_and(mom_y * y_coord, LXY - 1).astype(F32) / LXY
        beside = plane + 1 if at < BLOCKS // 2 else plane + z_length - 1
        for index, z_coord in enumerate((plane, beside)):
            part_z = jnp.bitwise_and(mom_z * z_coord, z_length - 1).astype(F32) / z_length
            theta = TWO_PI * (part_x + part_y + part_z)
            cosine[index, :, at * LANES : (at + 1) * LANES] = jnp.cos(theta)
            sine[index, :, at * LANES : (at + 1) * LANES] = jnp.sin(theta)


def make_blocks(side, raw, tiles, blocks):
    @pl.loop(0, side)
    def _(high):
        for low in range(side):
            start = pl.multiple_of((high * side + low) * PLANE, PLANE)
            plane = raw[:, pl.ds(start, PLANE)].astype(F32)
            for at in range(BLOCKS):
                row = (low * BLOCKS + at) * 8
                tiles[row : row + COMPS, :] = plane[:, at * LANES : (at + 1) * LANES]
            for comp in range(0, COMPS, 2):
                pieces = [
                    tiles[pl.ds(low * BLOCKS * 8 + c, BLOCKS, stride=8), :]
                    for c in (comp, comp + 1)
                ]
                blocks[high, low, comp * BLOCKS : (comp + 2) * BLOCKS, :] = jnp.concatenate(
                    pieces, axis=0
                ).astype(BF16)


def pack_links(links_ref, links_out, links_z_out):
    for at in range(BLOCKS):
        lanes = slice(at * LANES, (at + 1) * LANES)
        rows = [links_ref[direction, :, lanes].astype(F32) for direction in range(NDIR)]
        for direction in range(NDIR):
            links_out[at, direction * 24 : direction * 24 + 18, :] = rows[direction].astype(BF16)
        if at >= BLOCKS // 2:
            links_z_out[at - BLOCKS // 2, 0:18, :] = rows[2].astype(BF16)


def fill_tables(links, table):
    lane = lax.broadcasted_iota(jnp.int32, (1, LANES), 1)
    x_lane = jnp.bitwise_and(lane, LXY - 1)

    def block(index):
        return slice(index * LANES, (index + 1) * LANES)

    for direction in range(2):
        for at in range(BLOCKS):
            wide = 0.5 * links[at, direction * 24 : direction * 24 + 24, :].astype(F32)
            own = [wide[e : e + 1] for e in range(18)]
            if direction == 0:
                moved = [jnp.where(x_lane == 0, roll(u, 97), roll(u, 1)) for u in own]
            else:
                before = (at + BLOCKS - 1) % BLOCKS
                wide = 0.5 * links[before, direction * 24 : direction * 24 + 24, :].astype(F32)
                other = [wide[e : e + 1] for e in range(18)]
                moved = [
                    jnp.where(lane < LXY, roll(o, LXY), roll(u, LXY)) for o, u in zip(other, own)
                ]
            for e in range(18):
                table[2 * direction, e : e + 1, block(at)] = own[e]
            for e, value in enumerate(minus_adjoint(moved)):
                table[2 * direction + 1, e : e + 1, block(at)] = value


def fill_z_tables(links, links_z, table):
    for at in range(BLOCKS):
        lanes = slice(at * LANES, (at + 1) * LANES)
        if at < BLOCKS // 2:
            wide = 0.5 * links[at, 48:72, :].astype(F32)
            straight, turned = 4, 5
        else:
            wide = 0.5 * links_z[at - BLOCKS // 2, 0:24, :].astype(F32)
            straight, turned = 5, 4
        own = [wide[e : e + 1] for e in range(18)]
        for e in range(18):
            table[straight, e : e + 1, lanes] = own[e]
        for e, value in enumerate(minus_adjoint(own)):
            table[turned, e : e + 1, lanes] = value


def fill_order(core, side, order):
    bits = side.bit_length() - 1
    width = 2 * side * side
    row = lax.broadcasted_iota(jnp.int32, (width, width), 0)
    column = lax.broadcasted_iota(jnp.int32, (width, width), 1)
    low = jnp.bitwise_and(row, side - 1)
    place = jnp.bitwise_and(jnp.right_shift(row, bits), side - 1)
    rest = row - low - place * side
    high = jnp.right_shift(place, 1) + (side // 2) * jnp.bitwise_and(place, 1)
    number = jnp.where(core == 1, low * side + high, high * side + low)
    order[...] = jnp.where(column == rest + number, 1.0, 0.0)


def kernel(
    side, vectors_hbm, links_hbm, momenta_hbm, directions_hbm, out_ref,
    raw, tiles, x_ref, links_ref, momenta_ref, directions_ref,
    ra, rb, spread, field, field_b, halo, links_z_out, links, links_z, table, cosine, sine, order,
    twisted, twisted_h, twisted_h0, packed_xy, packed_z, packed_h, acc_xy, acc_z, send_xy, send_z, got_xy, got_z,
    sum_xy, sum_z, rows_out, rows_in,
    sem_i, ready, sem_a, sem_b, sem_h, sem_l, sem_r, sem_s,
):
    nev = side * side
    pairs = side // 2
    group = 2 * side
    me, core = lax.axis_index("space"), lax.axis_index("tm")
    high, low = me // side, me % side
    a = low + core * (high - low)
    b = high + core * (low - high)

    def device(at_a, at_b):
        return (1 - core) * (at_b * side + at_a) + core * (at_a * side + at_b)

    above = (me + 1) % nev
    below = (me + nev - 1) % nev

    barrier = pltpu.get_barrier_semaphore()

    def greet(target):
        pl.semaphore_signal(barrier, inc=1, device_id={"space": target}, device_id_type=MESH)

    def has_up(distance):
        return 1 - (b + distance) // side

    def has_down(distance):
        return (b + side - distance) // side

    def tell(distance, signal):
        @pl.when(has_up(distance) == 1)
        def _():
            signal(device(a, b + distance))

        @pl.when(has_down(distance) == 1)
        def _():
            signal(device(a, b - distance))

    for step in range(1, side):
        greet(device((a + step) % side, b))
    tell(1, greet)
    sources = (vectors_hbm, links_hbm, momenta_hbm, directions_hbm)
    targets = (raw, links_ref, momenta_ref, directions_ref)
    inputs = [
        pltpu.make_async_copy(source, target, sem_i.at[index])
        for index, (source, target) in enumerate(zip(sources, targets))
    ]
    for copy in inputs:
        copy.start()
    inputs[0].wait()
    make_blocks(side, raw, tiles, x_ref)
    inputs[1].wait()
    pack_links(links_ref, links, links_z_out)
    pl.semaphore_wait(barrier, side - 1 + has_up(1) + has_down(1))

    def send(src, dst, sent, arrived, target):
        copy = pltpu.make_async_remote_copy(
            src_ref=src, dst_ref=dst, send_sem=sent, recv_sem=arrived,
            device_id={"space": target}, device_id_type=MESH,
        )
        copy.start()
        return copy

    far_a = sorted(range(1, side), key=lambda k: -min(k, side - k))
    own_pair = b % pairs

    for step in far_a:
        to_a = (a + step) % side

        @pl.when(core == 0)
        def _():
            send(x_ref.at[:, to_a], ra.at[a], sem_s.at[2], sem_a, device(to_a, b))

        @pl.when(core == 1)
        def _():
            send(x_ref.at[to_a], ra.at[a], sem_s.at[2], sem_a, device(to_a, b))

    for to_b in range(side):
        ra[a, to_b] = x_ref[
            (1 - core) * to_b + core * a, (1 - core) * a + core * to_b
        ]
    inputs[2].wait()
    inputs[3].wait()
    fill_phases(momenta_ref, me, nev, cosine, sine)
    fill_order(core, side, order)
    fill_tables(links, table)

    for place in range(rounds_of(side)):

        def mark(target):
            pl.semaphore_signal(
                ready.at[place], inc=1, device_id={"space": target}, device_id_type=MESH
            )

        tell(2**place, mark)
        pl.semaphore_wait(ready.at[place], has_up(2**place) + has_down(2**place))

    links_copy = send(links_z_out, links_z, sem_s.at[1], sem_l, above)

    wait_for(ra.at[pl.ds(0, side - 1)], sem_a)
    for turn in reversed(range(pairs)):
        for member in range(2 if turn else 1):
            to_b = (b + turn) % pairs + member * pairs if turn else (b + pairs) % side
            send(ra.at[:, to_b], rb.at[b], sem_s.at[3], sem_b.at[own_pair], device(a, to_b))
    for from_a in range(side):
        rb[b, from_a] = ra[from_a, b]

    links_copy.wait()
    fill_z_tables(links, links_z, table)
    upper = pl.ds(HALF, HALF)
    lane = lax.broadcasted_iota(jnp.int32, (1, LANES), 1)
    x_lane = jnp.bitwise_and(lane, LXY - 1)
    lower_half = pl.ds(0, HALF)

    def own_arrive(pair):
        @pl.when(pair == own_pair)
        def _():
            wait_for(rb.at[pl.ds(0, 1)], sem_b.at[pair])

        @pl.when(pair != own_pair)
        def _():
            wait_for(rb.at[pl.ds(0, 2)], sem_b.at[pair])

        for member in range(2):
            for from_a in range(side):
                spread[pl.ds((member * side + from_a) * PITCH, BLOCK_ROWS), :] = rb[
                    pair + member * pairs, from_a
                ].astype(F32)
        for comp in range(COMPS):
            for at in range(BLOCKS):
                rows = spread[pl.ds(comp * BLOCKS + at, group, stride=PITCH), :]
                field[comp, :, at * LANES : (at + 1) * LANES] = rows
                field_b[pair, comp, :, at * LANES : (at + 1) * LANES] = rows.astype(BF16)
        send(
            field_b.at[pair, :, :, lower_half], halo.at[pair, :, :, lower_half],
            sem_s.at[4], sem_h.at[0, pair], below,
        )
        send(
            field_b.at[pair, :, :, upper], halo.at[pair, :, :, upper],
            sem_s.at[4], sem_h.at[1, pair], above,
        )


    def own_block(pair, at):
        rows_at = pl.multiple_of(pair * group, group)
        lanes = lanes_at(0, at)
        after = lanes_at(0, (at + 1) % BLOCKS)
        before = lanes_at(0, (at + BLOCKS - 1) % BLOCKS)
        vec = [field[c, :, lanes] for c in range(COMPS)]
        store_twisted(twisted, pair, group, at, cosine.at[0], sine.at[0], vec)
        ahead = [jnp.where(x_lane == LXY - 1, roll(v, 31), roll(v, 127)) for v in vec]
        behind = [jnp.where(x_lane == 0, roll(v, 97), roll(v, 1)) for v in vec]
        first = apply_table(table.at[0], lanes, ahead)
        second = apply_table(table.at[1], lanes, behind)
        store_packed(
            packed_xy, 0, 0, nev, rows_at, group, at, [f + s for f, s in zip(first, second)]
        )
        ahead = [
            jnp.where(lane < LANES - LXY, roll(v, 96), roll(field[c, :, after], 96))
            for c, v in enumerate(vec)
        ]
        behind = [
            jnp.where(lane < LXY, roll(field[c, :, before], LXY), roll(v, LXY))
            for c, v in enumerate(vec)
        ]
        first = apply_table(table.at[2], lanes, ahead)
        second = apply_table(table.at[3], lanes, behind)
        store_packed(
            packed_xy, 2 * nev, 0, nev, rows_at, group, at,
            [f + s for f, s in zip(first, second)],
        )
        store_packed(
            packed_h, 0, 0, nev, rows_at, group, at,
            apply_table(table.at[5], lanes, vec),
        )

    def own_plane(pair):
        own_arrive(pair)

        @pl.loop(0, BLOCKS)
        def _(at):
            own_block(pair, at)

    def halo_wait(which):
        for pair in which:
            wait_for(halo.at[0, :, :, lower_half], sem_h.at[0, pair])
            wait_for(halo.at[0, :, :, upper], sem_h.at[1, pair])

    def beside_block(target, place, pair, at):
        rows_at = pair * group
        lanes = lanes_at(0, at)
        vec = [halo[pair, c, :, lanes].astype(F32) for c in range(COMPS)]
        store_twisted(target, place, group, at, cosine.at[1], sine.at[1], vec)
        store_packed(
            packed_z, 0, 0, nev, rows_at, group, at, apply_table(table.at[4], lanes, vec)
        )

    def spread_sums(acc, parts, outgoing, got, sent, sem):
        width = 2 * NMOM
        for to_a in range(side):
            for index in range(parts):
                for pair in range(pairs):
                    at = (index * pairs + pair) * width
                    outgoing[to_a, at : at + width, :] = acc[
                        index, pl.ds(pair * NMOM * group + to_a, width, stride=side), :
                    ].astype(BF16)
        for step in far_a:
            to_a = (a + step) % side
            send(outgoing.at[to_a], got.at[step - 1], sent, sem, device(to_a, b))

    def collect_sums(outgoing, got, total, sem):
        wait_for(got, sem)
        value = outgoing[a].astype(F32)
        for index in range(side - 1):
            value = value + got[index].astype(F32)
        total[...] = value

    for index in range(pairs - 1):
        own_plane(1 + (index + own_pair) % (pairs - 1))
    own_plane(0)
    halo_wait(range(1, pairs))
    acc_xy[...] = jnp.zeros_like(acc_xy)
    acc_z[...] = jnp.zeros_like(acc_z)

    def chunks(half):
        for slot in range(COMPS):
            yield pl.ds(pl.multiple_of(slot * PLANE + half * 2 * LANES, 2 * LANES), 2 * LANES)

    @pl.loop(0, BLOCKS // 2)
    def _(half):
        total = None
        for part in chunks(half):
            product = contract(twisted[:, part], packed_xy[:, part])
            total = product if total is None else total + product
        for index in range(2):
            acc_xy[index] += total[:, index * 2 * nev : (index + 1) * 2 * nev]
        for pair in range(1, pairs):
            for at in range(2):
                beside_block(twisted_h, pair - 1, pair, 2 * half + at)

    spread_sums(acc_xy, 2, send_xy, got_xy, sem_s.at[5], sem_r.at[0])
    halo_wait([0])
    early = slice(NMOM * group, NMOM * nev)
    late = slice(0, NMOM * group)

    @pl.loop(0, BLOCKS // 2)
    def _(half):
        total = None
        for part in chunks(half):
            product = contract(twisted_h[:, part], packed_h[:, part])
            total = product if total is None else total + product
        acc_z[0, early, :] += total
        for at in range(2):
            beside_block(twisted_h0, 0, 0, 2 * half + at)

    acc_z[0, late, :] = contract(twisted_h0[...], packed_h[...])
    acc_z[0] += contract(twisted[...], packed_z[...])
    spread_sums(acc_z, 1, send_z, got_z, sem_s.at[6], sem_r.at[1])

    collect_sums(send_xy, got_xy, sum_xy, sem_r.at[0])
    collect_sums(send_z, got_z, sum_z, sem_r.at[1])
    for place in range(side):
        first = (place // 2) * 2 * NMOM + place % 2
        for index, total in enumerate((sum_xy, sum_xy, sum_z)):
            start = first + (index % 2) * NMOM * side
            rows_out[place, index * NMOM : (index + 1) * NMOM, :] = total[
                pl.ds(start, NMOM, stride=2), :
            ]

    def place_of(at_b):
        return 2 * (at_b % pairs) + at_b // pairs

    for step in far_a:
        to_b = (b + step) % side
        send(rows_out.at[place_of(to_b)], rows_in.at[step - 1], sem_s.at[7], sem_r.at[2], device(a, to_b))
    wait_for(rows_in, sem_r.at[2])
    value = rows_out[place_of(b)]
    for index in range(side - 1):
        value = value + rows_in[index]
    last = jnp.dot(value, order[...], preferred_element_type=F32, precision=lax.Precision.HIGHEST)
    by_dir = [last[index * NMOM : (index + 1) * NMOM] for index in range(NDIR)]
    for slot in range(NDIR):
        chosen = directions_ref[slot]
        out_ref[slot] = jnp.where(
            chosen == 0, by_dir[0], jnp.where(chosen == 1, by_dir[1], by_dir[2])
        )

    wait_for(ra.at[pl.ds(0, side - 1)], sem_s.at[2])
    wait_for(rb.at[pl.ds(0, side - 1)], sem_s.at[3])
    wait_for(field_b, sem_s.at[4])
    wait_for(got_xy, sem_s.at[5])
    wait_for(got_z, sem_s.at[6])
    wait_for(rows_in, sem_s.at[7])


def shards(vectors, gauge_links, momenta, directions):
    space = lax.axis_size("space")
    side = math.isqrt(space)
    nev, pairs, group = space, side // 2, 2 * side
    scratch = [
        ((COMPS, space * PLANE), BF16),
        ((side * BLOCKS * 8, LANES), F32),
        ((side, side, BLOCK_ROWS, LANES), BF16),
        ((NDIR, 18, PLANE), BF16),
        ((side, side, BLOCK_ROWS, LANES), BF16),
        ((side, side, BLOCK_ROWS, LANES), BF16),
        ((group * PITCH, LANES), F32),
        ((COMPS, group, PLANE), F32),
        ((pairs, COMPS, group, PLANE), BF16),
        ((pairs, COMPS, group, PLANE), BF16),
        ((BLOCKS // 2, 32, LANES), BF16),
        ((BLOCKS, 80, LANES), BF16),
        ((BLOCKS // 2, 32, LANES), BF16),
        ((6, 24, PLANE), F32),
        ((2, NMOM, PLANE), F32),
        ((2, NMOM, PLANE), F32),
        ((2 * nev, 2 * nev), F32),
        ((NMOM * nev, DEPTH), BF16),
        ((NMOM * (nev - group), DEPTH), BF16),
        ((NMOM * group, DEPTH), BF16),
        ((4 * nev, DEPTH), BF16),
        ((2 * nev, DEPTH), BF16),
        ((2 * nev, DEPTH), BF16),
        ((2, NMOM * nev, 2 * nev), F32),
        ((1, NMOM * nev, 2 * nev), F32),
        ((side, 2 * NMOM * side, 2 * nev), BF16),
        ((side, NMOM * side, 2 * nev), BF16),
        ((side - 1, 2 * NMOM * side, 2 * nev), BF16),
        ((side - 1, NMOM * side, 2 * nev), BF16),
        ((2 * NMOM * side, 2 * nev), F32),
        ((NMOM * side, 2 * nev), F32),
        ((side, NDIR * NMOM, 2 * nev), F32),
        ((side - 1, NDIR * NMOM, 2 * nev), F32),
    ]
    dma = pltpu.SemaphoreType.DMA
    out = pl.pallas_call(
        functools.partial(kernel, side),
        out_shape=jax.ShapeDtypeStruct((NDIR, NMOM, 2 * nev), F32),
        in_specs=[pl.BlockSpec(memory_space=pl.ANY)] * 4,
        out_specs=pl.BlockSpec(memory_space=pltpu.VMEM),
        scratch_shapes=[pltpu.VMEM(*s) for s in scratch[:4]]
        + [pltpu.SMEM((NDIR, NMOM), jnp.int32), pltpu.SMEM((NDIR,), jnp.int32)]
        + [pltpu.VMEM(*s) for s in scratch[4:]]
        + [dma((4,))]
        + [pltpu.SemaphoreType.REGULAR((max(1, rounds_of(side)),))]
        + [dma, dma((pairs,)), dma((2, pairs)), dma, dma((3,)), dma((8,))],
        compiler_params=pltpu.CompilerParams(
            collective_id=0, has_side_effects=True, vmem_limit_bytes=60 * 1024 * 1024
        ),
    )(vectors[0, 0], gauge_links[0], momenta.T, directions)
    return jnp.transpose(out, (1, 0, 2))[None, None]


def solution(mesh):
    return jax.shard_map(
        shards,
        mesh=mesh,
        in_specs=(
            P(("cfg", "tm"), "space", None, None),
            P(("cfg", "tm"), None, None, "space"),
            P(),
            P(),
        ),
        out_specs=P("space", ("cfg", "tm"), None, None, None),
        check_vma=False,
    )
```

```python
import functools
import math

import jax
import jax.numpy as jnp
from jax import lax
from jax.experimental import pallas as pl
from jax.experimental.pallas import tpu as pltpu
from jax.sharding import PartitionSpec as P

LXY = 32
NMOM = 8
NDIR = 3
PLANE = LXY * LXY
LANES = 128
BLOCKS = PLANE // LANES
HALF = PLANE // 2
COMPS = 6
BLOCK_ROWS = COMPS * BLOCKS
PITCH = BLOCK_ROWS + 8
DEPTH = COMPS * PLANE
TWO_PI = 2.0 * math.pi
MESH = pl.DeviceIdType.MESH
BF16, F32 = jnp.bfloat16, jnp.float32


def roll(value, shift):
    return pltpu.roll(value, shift, value.ndim - 1)


def apply_table(table, lanes, field):
    out_re, out_im = [], []
    for row in range(3):
        acc_re = acc_im = None
        for col in range(3):
            link_re = table[3 * row + col : 3 * row + col + 1, lanes]
            link_im = table[9 + 3 * row + col : 10 + 3 * row + col, lanes]
            re = link_re * field[col] - link_im * field[3 + col]
            im = link_re * field[3 + col] + link_im * field[col]
            acc_re = re if acc_re is None else acc_re + re
            acc_im = im if acc_im is None else acc_im + im
        out_re.append(acc_re)
        out_im.append(acc_im)
    return out_re + out_im


def minus_adjoint(entries):
    real = [-entries[3 * b + a] for a in range(3) for b in range(3)]
    imag = [entries[9 + 3 * b + a] for a in range(3) for b in range(3)]
    return real + imag


def lanes_at(slot, at):
    return pl.ds(pl.multiple_of(slot * PLANE + at * LANES, LANES), LANES)


def store_packed(packed, base, first, nev, rows_at, group, at, value):
    for colour in range(3):
        re = value[colour].astype(BF16)
        im = value[3 + colour].astype(BF16)
        upper, lower = pl.ds(base + rows_at, group), pl.ds(base + nev + rows_at, group)
        packed[upper, lanes_at(first + colour, at)] = re
        packed[lower, lanes_at(first + colour, at)] = im
        packed[upper, lanes_at(first + 3 + colour, at)] = im
        packed[lower, lanes_at(first + 3 + colour, at)] = -re


def store_twisted(twisted, pair, group, at, cosine, sine, field):
    for mom in range(NMOM):
        cos_row = cosine[mom : mom + 1, lanes_at(0, at)]
        sin_row = sine[mom : mom + 1, lanes_at(0, at)]
        rows = pl.ds(pl.multiple_of(pair * NMOM * group, group) + mom * group, group)
        for colour in range(3):
            vec_re, vec_im = field[colour], field[3 + colour]
            twisted[rows, lanes_at(colour, at)] = (
                vec_re * cos_row - vec_im * sin_row
            ).astype(BF16)
            twisted[rows, lanes_at(3 + colour, at)] = (
                vec_re * sin_row + vec_im * cos_row
            ).astype(BF16)


def contract(left, right):
    return lax.dot_general(left, right, (((1,), (1,)), ((), ())), preferred_element_type=F32)


def wait_for(ref, sem):
    pltpu.make_async_copy(ref, ref, sem).wait()


def fill_phases(momenta, plane, z_length, cosine, sine):
    row = lax.broadcasted_iota(jnp.int32, (NMOM, LANES), 0)
    lane = lax.broadcasted_iota(jnp.int32, (NMOM, LANES), 1)

    def column(axis):
        value = jnp.zeros((NMOM, LANES), jnp.int32)
        for mom in range(NMOM):
            value = jnp.where(row == mom, momenta[axis, mom], value)
        return value

    mom_x, mom_y, mom_z = column(0), column(1), column(2)
    part_x = jnp.bitwise_and(mom_x * jnp.bitwise_and(lane, LXY - 1), LXY - 1).astype(F32) / LXY
    y_low = jnp.right_shift(lane, LXY.bit_length() - 1)
    for at in range(BLOCKS):
        y_coord = y_low + at * (LANES // LXY)
        part_y = jnp.bitwise_and(mom_y * y_coord, LXY - 1).astype(F32) / LXY
        beside = plane + 1 if at < BLOCKS // 2 else plane + z_length - 1
        for index, z_coord in enumerate((plane, beside)):
            part_z = jnp.bitwise_and(mom_z * z_coord, z_length - 1).astype(F32) / z_length
            theta = TWO_PI * (part_x + part_y + part_z)
            cosine[index, :, at * LANES : (at + 1) * LANES] = jnp.cos(theta)
            sine[index, :, at * LANES : (at + 1) * LANES] = jnp.sin(theta)


def make_blocks(side, raw, tiles, blocks):
    @pl.loop(0, side)
    def _(high):
        for low in range(side):
            start = pl.multiple_of((high * side + low) * PLANE, PLANE)
            plane = raw[:, pl.ds(start, PLANE)].astype(F32)
            for at in range(BLOCKS):
                row = (low * BLOCKS + at) * 8
                tiles[row : row + COMPS, :] = plane[:, at * LANES : (at + 1) * LANES]
            for comp in range(0, COMPS, 2):
                pieces = [
                    tiles[pl.ds(low * BLOCKS * 8 + c, BLOCKS, stride=8), :]
                    for c in (comp, comp + 1)
                ]
                blocks[high, low, comp * BLOCKS : (comp + 2) * BLOCKS, :] = jnp.concatenate(
                    pieces, axis=0
                ).astype(BF16)


def pack_links(links_ref, links_out, links_z_out):
    for at in range(BLOCKS):
        lanes = slice(at * LANES, (at + 1) * LANES)
        rows = [links_ref[direction, :, lanes].astype(F32) for direction in range(NDIR)]
        for direction in range(NDIR):
            links_out[at, direction * 24 : direction * 24 + 18, :] = rows[direction].astype(BF16)
        if at >= BLOCKS // 2:
            links_z_out[at - BLOCKS // 2, 0:18, :] = rows[2].astype(BF16)


def fill_tables(links, table):
    lane = lax.broadcasted_iota(jnp.int32, (1, LANES), 1)
    x_lane = jnp.bitwise_and(lane, LXY - 1)

    def block(index):
        return slice(index * LANES, (index + 1) * LANES)

    for direction in range(2):
        for at in range(BLOCKS):
            wide = 0.5 * links[at, direction * 24 : direction * 24 + 24, :].astype(F32)
            own = [wide[e : e + 1] for e in range(18)]
            if direction == 0:
                moved = [jnp.where(x_lane == 0, roll(u, 97), roll(u, 1)) for u in own]
            else:
                before = (at + BLOCKS - 1) % BLOCKS
                wide = 0.5 * links[before, direction * 24 : direction * 24 + 24, :].astype(F32)
                other = [wide[e : e + 1] for e in range(18)]
                moved = [
                    jnp.where(lane < LXY, roll(o, LXY), roll(u, LXY)) for o, u in zip(other, own)
                ]
            for e in range(18):
                table[2 * direction, e : e + 1, block(at)] = own[e]
            for e, value in enumerate(minus_adjoint(moved)):
                table[2 * direction + 1, e : e + 1, block(at)] = value


def fill_z_tables(links, links_z, table):
    for at in range(BLOCKS):
        lanes = slice(at * LANES, (at + 1) * LANES)
        if at < BLOCKS // 2:
            wide = 0.5 * links[at, 48:72, :].astype(F32)
            straight, turned = 4, 5
        else:
            wide = 0.5 * links_z[at - BLOCKS // 2, 0:24, :].astype(F32)
            straight, turned = 5, 4
        own = [wide[e : e + 1] for e in range(18)]
        for e in range(18):
            table[straight, e : e + 1, lanes] = own[e]
        for e, value in enumerate(minus_adjoint(own)):
            table[turned, e : e + 1, lanes] = value


def fill_order(core, side, order):
    bits = side.bit_length() - 1
    width = 2 * side * side
    row = lax.broadcasted_iota(jnp.int32, (width, width), 0)
    column = lax.broadcasted_iota(jnp.int32, (width, width), 1)
    low = jnp.bitwise_and(row, side - 1)
    place = jnp.bitwise_and(jnp.right_shift(row, bits), side - 1)
    rest = row - low - place * side
    high = jnp.right_shift(place, 1) + (side // 2) * jnp.bitwise_and(place, 1)
    number = jnp.where(core == 1, low * side + high, high * side + low)
    order[...] = jnp.where(column == rest + number, 1.0, 0.0)


def kernel(
    side, vectors_hbm, links_hbm, momenta_hbm, directions_hbm, out_ref,
    raw, tiles, x_ref, links_ref, momenta_ref, directions_ref,
    ra, rb, spread, field, field_b, halo, links_z_out, links, links_z, table, cosine, sine, order,
    twisted, twisted_h, twisted_h0, packed_xy, packed_z, packed_h, acc_xy, acc_z, send_xy, send_z, got_xy, got_z,
    sum_xy, sum_z, rows_out, rows_in,
    sem_i, ready, sem_a, sem_b, sem_h, sem_l, sem_r, sem_s,
):
    nev = side * side
    pairs = side // 2
    group = 2 * side
    me, core = lax.axis_index("space"), lax.axis_index("tm")
    high, low = me // side, me % side
    a = low + core * (high - low)
    b = high + core * (low - high)

    def device(at_a, at_b):
        return (1 - core) * (at_b * side + at_a) + core * (at_a * side + at_b)

    above = (me + 1) % nev
    below = (me + nev - 1) % nev

    barrier = pltpu.get_barrier_semaphore()

    def greet(target):
        pl.semaphore_signal(barrier, inc=1, device_id={"space": target}, device_id_type=MESH)

    beside_b = (device(a, (b + 1) % side), device(a, (b + side - 1) % side))
    for step in range(1, side):
        greet(device((a + step) % side, b))
    for target in (above, below) + beside_b:
        greet(target)
    sources = (vectors_hbm, links_hbm, momenta_hbm, directions_hbm)
    targets = (raw, links_ref, momenta_ref, directions_ref)
    inputs = [
        pltpu.make_async_copy(source, target, sem_i.at[index])
        for index, (source, target) in enumerate(zip(sources, targets))
    ]
    for copy in inputs:
        copy.start()
    inputs[0].wait()
    make_blocks(side, raw, tiles, x_ref)
    inputs[1].wait()
    pack_links(links_ref, links, links_z_out)
    pl.semaphore_wait(barrier, side - 1 + 4)

    def send(src, dst, sent, arrived, target):
        copy = pltpu.make_async_remote_copy(
            src_ref=src, dst_ref=dst, send_sem=sent, recv_sem=arrived,
            device_id={"space": target}, device_id_type=MESH,
        )
        copy.start()
        return copy

    far_a = sorted(range(1, side), key=lambda k: -min(k, side - k))
    own_pair = b % pairs

    for step in far_a:
        to_a = (a + step) % side

        @pl.when(core == 0)
        def _():
            send(x_ref.at[:, to_a], ra.at[a], sem_s.at[2], sem_a, device(to_a, b))

        @pl.when(core == 1)
        def _():
            send(x_ref.at[to_a], ra.at[a], sem_s.at[2], sem_a, device(to_a, b))

    links_copy = send(links_z_out, links_z, sem_s.at[1], sem_l, above)
    for to_b in range(side):
        ra[a, to_b] = x_ref[
            (1 - core) * to_b + core * a, (1 - core) * a + core * to_b
        ]
    inputs[2].wait()
    inputs[3].wait()
    fill_phases(momenta_ref, me, nev, cosine, sine)
    fill_order(core, side, order)
    fill_tables(links, table)

    for place in range(side // 2 - 1):
        for target in beside_b:
            pl.semaphore_signal(
                ready.at[place], inc=1, device_id={"space": target}, device_id_type=MESH
            )
        pl.semaphore_wait(ready.at[place], 2)

    wait_for(ra.at[pl.ds(0, side - 1)], sem_a)
    for turn in reversed(range(pairs)):
        for member in range(2 if turn else 1):
            to_b = (b + turn) % pairs + member * pairs if turn else (b + pairs) % side
            send(ra.at[:, to_b], rb.at[b], sem_s.at[3], sem_b.at[own_pair], device(a, to_b))
    for from_a in range(side):
        rb[b, from_a] = ra[from_a, b]

    links_copy.wait()
    fill_z_tables(links, links_z, table)
    upper = pl.ds(HALF, HALF)
    lane = lax.broadcasted_iota(jnp.int32, (1, LANES), 1)
    x_lane = jnp.bitwise_and(lane, LXY - 1)
    lower_half = pl.ds(0, HALF)

    def own_arrive(pair):
        @pl.when(pair == own_pair)
        def _():
            wait_for(rb.at[pl.ds(0, 1)], sem_b.at[pair])

        @pl.when(pair != own_pair)
        def _():
            wait_for(rb.at[pl.ds(0, 2)], sem_b.at[pair])

        for member in range(2):
            for from_a in range(side):
                spread[pl.ds((member * side + from_a) * PITCH, BLOCK_ROWS), :] = rb[
                    pair + member * pairs, from_a
                ].astype(F32)
        for comp in range(COMPS):
            for at in range(BLOCKS):
                rows = spread[pl.ds(comp * BLOCKS + at, group, stride=PITCH), :]
                field[comp, :, at * LANES : (at + 1) * LANES] = rows
                field_b[pair, comp, :, at * LANES : (at + 1) * LANES] = rows.astype(BF16)
        send(
            field_b.at[pair, :, :, lower_half], halo.at[pair, :, :, lower_half],
            sem_s.at[4], sem_h.at[0, pair], below,
        )
        send(
            field_b.at[pair, :, :, upper], halo.at[pair, :, :, upper],
            sem_s.at[4], sem_h.at[1, pair], above,
        )


    def own_block(pair, at):
        rows_at = pl.multiple_of(pair * group, group)
        lanes = lanes_at(0, at)
        after = lanes_at(0, (at + 1) % BLOCKS)
        before = lanes_at(0, (at + BLOCKS - 1) % BLOCKS)
        vec = [field[c, :, lanes] for c in range(COMPS)]
        store_twisted(twisted, pair, group, at, cosine.at[0], sine.at[0], vec)
        ahead = [jnp.where(x_lane == LXY - 1, roll(v, 31), roll(v, 127)) for v in vec]
        behind = [jnp.where(x_lane == 0, roll(v, 97), roll(v, 1)) for v in vec]
        first = apply_table(table.at[0], lanes, ahead)
        second = apply_table(table.at[1], lanes, behind)
        store_packed(
            packed_xy, 0, 0, nev, rows_at, group, at, [f + s for f, s in zip(first, second)]
        )
        ahead = [
            jnp.where(lane < LANES - LXY, roll(v, 96), roll(field[c, :, after], 96))
            for c, v in enumerate(vec)
        ]
        behind = [
            jnp.where(lane < LXY, roll(field[c, :, before], LXY), roll(v, LXY))
            for c, v in enumerate(vec)
        ]
        first = apply_table(table.at[2], lanes, ahead)
        second = apply_table(table.at[3], lanes, behind)
        store_packed(
            packed_xy, 2 * nev, 0, nev, rows_at, group, at,
            [f + s for f, s in zip(first, second)],
        )
        store_packed(
            packed_h, 0, 0, nev, rows_at, group, at,
            apply_table(table.at[5], lanes, vec),
        )

    def own_plane(pair):
        own_arrive(pair)

        @pl.loop(0, BLOCKS)
        def _(at):
            own_block(pair, at)

    def halo_wait(which):
        for pair in which:
            wait_for(halo.at[0, :, :, lower_half], sem_h.at[0, pair])
            wait_for(halo.at[0, :, :, upper], sem_h.at[1, pair])

    def beside_block(target, place, pair, at):
        rows_at = pair * group
        lanes = lanes_at(0, at)
        vec = [halo[pair, c, :, lanes].astype(F32) for c in range(COMPS)]
        store_twisted(target, place, group, at, cosine.at[1], sine.at[1], vec)
        store_packed(
            packed_z, 0, 0, nev, rows_at, group, at, apply_table(table.at[4], lanes, vec)
        )

    def spread_sums(acc, parts, outgoing, got, sent, sem):
        width = 2 * NMOM
        for to_a in range(side):
            for index in range(parts):
                for pair in range(pairs):
                    at = (index * pairs + pair) * width
                    outgoing[to_a, at : at + width, :] = acc[
                        index, pl.ds(pair * NMOM * group + to_a, width, stride=side), :
                    ].astype(BF16)
        for step in far_a:
            to_a = (a + step) % side
            send(outgoing.at[to_a], got.at[step - 1], sent, sem, device(to_a, b))

    def collect_sums(outgoing, got, total, sem):
        wait_for(got, sem)
        value = outgoing[a].astype(F32)
        for index in range(side - 1):
            value = value + got[index].astype(F32)
        total[...] = value

    for index in range(pairs - 1):
        own_plane(1 + (index + own_pair) % (pairs - 1))
    own_plane(0)
    halo_wait(range(1, pairs))
    acc_xy[...] = jnp.zeros_like(acc_xy)
    acc_z[...] = jnp.zeros_like(acc_z)

    def chunks(half):
        for slot in range(COMPS):
            yield pl.ds(pl.multiple_of(slot * PLANE + half * 2 * LANES, 2 * LANES), 2 * LANES)

    @pl.loop(0, BLOCKS // 2)
    def _(half):
        total = None
        for part in chunks(half):
            product = contract(twisted[:, part], packed_xy[:, part])
            total = product if total is None else total + product
        for index in range(2):
            acc_xy[index] += total[:, index * 2 * nev : (index + 1) * 2 * nev]
        for pair in range(1, pairs):
            for at in range(2):
                beside_block(twisted_h, pair - 1, pair, 2 * half + at)

    spread_sums(acc_xy, 2, send_xy, got_xy, sem_s.at[5], sem_r.at[0])
    halo_wait([0])
    early = slice(NMOM * group, NMOM * nev)
    late = slice(0, NMOM * group)

    @pl.loop(0, BLOCKS // 2)
    def _(half):
        total = None
        for part in chunks(half):
            product = contract(twisted_h[:, part], packed_h[:, part])
            total = product if total is None else total + product
        acc_z[0, early, :] += total
        for at in range(2):
            beside_block(twisted_h0, 0, 0, 2 * half + at)

    acc_z[0, late, :] = contract(twisted_h0[...], packed_h[...])
    acc_z[0] += contract(twisted[...], packed_z[...])
    spread_sums(acc_z, 1, send_z, got_z, sem_s.at[6], sem_r.at[1])

    collect_sums(send_xy, got_xy, sum_xy, sem_r.at[0])
    collect_sums(send_z, got_z, sum_z, sem_r.at[1])
    for place in range(side):
        first = (place // 2) * 2 * NMOM + place % 2
        for index, total in enumerate((sum_xy, sum_xy, sum_z)):
            start = first + (index % 2) * NMOM * side
            rows_out[place, index * NMOM : (index + 1) * NMOM, :] = total[
                pl.ds(start, NMOM, stride=2), :
            ]

    def place_of(at_b):
        return 2 * (at_b % pairs) + at_b // pairs

    for step in far_a:
        to_b = (b + step) % side
        send(rows_out.at[place_of(to_b)], rows_in.at[step - 1], sem_s.at[7], sem_r.at[2], device(a, to_b))
    wait_for(rows_in, sem_r.at[2])
    value = rows_out[place_of(b)]
    for index in range(side - 1):
        value = value + rows_in[index]
    last = jnp.dot(value, order[...], preferred_element_type=F32, precision=lax.Precision.HIGHEST)
    by_dir = [last[index * NMOM : (index + 1) * NMOM] for index in range(NDIR)]
    for slot in range(NDIR):
        chosen = directions_ref[slot]
        out_ref[slot] = jnp.where(
            chosen == 0, by_dir[0], jnp.where(chosen == 1, by_dir[1], by_dir[2])
        )

    wait_for(ra.at[pl.ds(0, side - 1)], sem_s.at[2])
    wait_for(rb.at[pl.ds(0, side - 1)], sem_s.at[3])
    wait_for(field_b, sem_s.at[4])
    wait_for(got_xy, sem_s.at[5])
    wait_for(got_z, sem_s.at[6])
    wait_for(rows_in, sem_s.at[7])


def shards(vectors, gauge_links, momenta, directions):
    space = lax.axis_size("space")
    side = math.isqrt(space)
    nev, pairs, group = space, side // 2, 2 * side
    scratch = [
        ((COMPS, space * PLANE), BF16),
        ((side * BLOCKS * 8, LANES), F32),
        ((side, side, BLOCK_ROWS, LANES), BF16),
        ((NDIR, 18, PLANE), BF16),
        ((side, side, BLOCK_ROWS, LANES), BF16),
        ((side, side, BLOCK_ROWS, LANES), BF16),
        ((group * PITCH, LANES), F32),
        ((COMPS, group, PLANE), F32),
        ((pairs, COMPS, group, PLANE), BF16),
        ((pairs, COMPS, group, PLANE), BF16),
        ((BLOCKS // 2, 32, LANES), BF16),
        ((BLOCKS, 80, LANES), BF16),
        ((BLOCKS // 2, 32, LANES), BF16),
        ((6, 24, PLANE), F32),
        ((2, NMOM, PLANE), F32),
        ((2, NMOM, PLANE), F32),
        ((2 * nev, 2 * nev), F32),
        ((NMOM * nev, DEPTH), BF16),
        ((NMOM * (nev - group), DEPTH), BF16),
        ((NMOM * group, DEPTH), BF16),
        ((4 * nev, DEPTH), BF16),
        ((2 * nev, DEPTH), BF16),
        ((2 * nev, DEPTH), BF16),
        ((2, NMOM * nev, 2 * nev), F32),
        ((1, NMOM * nev, 2 * nev), F32),
        ((side, 2 * NMOM * side, 2 * nev), BF16),
        ((side, NMOM * side, 2 * nev), BF16),
        ((side - 1, 2 * NMOM * side, 2 * nev), BF16),
        ((side - 1, NMOM * side, 2 * nev), BF16),
        ((2 * NMOM * side, 2 * nev), F32),
        ((NMOM * side, 2 * nev), F32),
        ((side, NDIR * NMOM, 2 * nev), F32),
        ((side - 1, NDIR * NMOM, 2 * nev), F32),
    ]
    dma = pltpu.SemaphoreType.DMA
    out = pl.pallas_call(
        functools.partial(kernel, side),
        out_shape=jax.ShapeDtypeStruct((NDIR, NMOM, 2 * nev), F32),
        in_specs=[pl.BlockSpec(memory_space=pl.ANY)] * 4,
        out_specs=pl.BlockSpec(memory_space=pltpu.VMEM),
        scratch_shapes=[pltpu.VMEM(*s) for s in scratch[:4]]
        + [pltpu.SMEM((NDIR, NMOM), jnp.int32), pltpu.SMEM((NDIR,), jnp.int32)]
        + [pltpu.VMEM(*s) for s in scratch[4:]]
        + [dma((4,))]
        + [pltpu.SemaphoreType.REGULAR((max(1, side // 2 - 1),))]
        + [dma, dma((pairs,)), dma((2, pairs)), dma, dma((3,)), dma((8,))],
        compiler_params=pltpu.CompilerParams(
            collective_id=0, has_side_effects=True, vmem_limit_bytes=60 * 1024 * 1024
        ),
    )(vectors[0, 0], gauge_links[0], momenta.T, directions)
    return jnp.transpose(out, (1, 0, 2))[None, None]


def solution(mesh):
    return jax.shard_map(
        shards,
        mesh=mesh,
        in_specs=(
            P(("cfg", "tm"), "space", None, None),
            P(("cfg", "tm"), None, None, "space"),
            P(),
            P(),
        ),
        out_specs=P("space", ("cfg", "tm"), None, None, None),
        check_vma=False,
    )
```

```python
import functools
import math

import jax
import jax.numpy as jnp
from jax import lax
from jax.experimental import pallas as pl
from jax.experimental.pallas import tpu as pltpu
from jax.sharding import PartitionSpec as P

LXY = 32
NMOM = 8
NDIR = 3
PLANE = LXY * LXY
LANES = 128
BLOCKS = PLANE // LANES
HALF = PLANE // 2
COMPS = 6
BLOCK_ROWS = COMPS * BLOCKS
PITCH = BLOCK_ROWS + 8
DEPTH = COMPS * PLANE
TWO_PI = 2.0 * math.pi
MESH = pl.DeviceIdType.MESH
BF16, F32 = jnp.bfloat16, jnp.float32


def roll(value, shift):
    return pltpu.roll(value, shift, value.ndim - 1)


def apply_table(table, lanes, field):
    out_re, out_im = [], []
    for row in range(3):
        acc_re = acc_im = None
        for col in range(3):
            link_re = table[3 * row + col : 3 * row + col + 1, lanes]
            link_im = table[9 + 3 * row + col : 10 + 3 * row + col, lanes]
            re = link_re * field[col] - link_im * field[3 + col]
            im = link_re * field[3 + col] + link_im * field[col]
            acc_re = re if acc_re is None else acc_re + re
            acc_im = im if acc_im is None else acc_im + im
        out_re.append(acc_re)
        out_im.append(acc_im)
    return out_re + out_im


def minus_adjoint(entries):
    real = [-entries[3 * b + a] for a in range(3) for b in range(3)]
    imag = [entries[9 + 3 * b + a] for a in range(3) for b in range(3)]
    return real + imag


def lanes_at(slot, at):
    return pl.ds(pl.multiple_of(slot * PLANE + at * LANES, LANES), LANES)


def store_packed(packed, base, first, nev, rows_at, group, at, value):
    for colour in range(3):
        re = value[colour].astype(BF16)
        im = value[3 + colour].astype(BF16)
        upper, lower = pl.ds(base + rows_at, group), pl.ds(base + nev + rows_at, group)
        packed[upper, lanes_at(first + colour, at)] = re
        packed[lower, lanes_at(first + colour, at)] = im
        packed[upper, lanes_at(first + 3 + colour, at)] = im
        packed[lower, lanes_at(first + 3 + colour, at)] = -re


def store_twisted(twisted, pair, group, at, cosine, sine, field):
    for mom in range(NMOM):
        cos_row = cosine[mom : mom + 1, lanes_at(0, at)]
        sin_row = sine[mom : mom + 1, lanes_at(0, at)]
        rows = pl.ds(pl.multiple_of(pair * NMOM * group, group) + mom * group, group)
        for colour in range(3):
            vec_re, vec_im = field[colour], field[3 + colour]
            twisted[rows, lanes_at(colour, at)] = (
                vec_re * cos_row - vec_im * sin_row
            ).astype(BF16)
            twisted[rows, lanes_at(3 + colour, at)] = (
                vec_re * sin_row + vec_im * cos_row
            ).astype(BF16)


def contract(left, right):
    return lax.dot_general(left, right, (((1,), (1,)), ((), ())), preferred_element_type=F32)


def wait_for(ref, sem):
    pltpu.make_async_copy(ref, ref, sem).wait()


def fill_phases(momenta, plane, z_length, cosine, sine):
    row = lax.broadcasted_iota(jnp.int32, (NMOM, LANES), 0)
    lane = lax.broadcasted_iota(jnp.int32, (NMOM, LANES), 1)

    def column(axis):
        value = jnp.zeros((NMOM, LANES), jnp.int32)
        for mom in range(NMOM):
            value = jnp.where(row == mom, momenta[axis, mom], value)
        return value

    mom_x, mom_y, mom_z = column(0), column(1), column(2)
    part_x = jnp.bitwise_and(mom_x * jnp.bitwise_and(lane, LXY - 1), LXY - 1).astype(F32) / LXY
    y_low = jnp.right_shift(lane, LXY.bit_length() - 1)
    for at in range(BLOCKS):
        y_coord = y_low + at * (LANES // LXY)
        part_y = jnp.bitwise_and(mom_y * y_coord, LXY - 1).astype(F32) / LXY
        beside = plane + 1 if at < BLOCKS // 2 else plane + z_length - 1
        for index, z_coord in enumerate((plane, beside)):
            part_z = jnp.bitwise_and(mom_z * z_coord, z_length - 1).astype(F32) / z_length
            theta = TWO_PI * (part_x + part_y + part_z)
            cosine[index, :, at * LANES : (at + 1) * LANES] = jnp.cos(theta)
            sine[index, :, at * LANES : (at + 1) * LANES] = jnp.sin(theta)


def make_blocks(side, raw, tiles, blocks):
    @pl.loop(0, side)
    def _(high):
        for low in range(side):
            start = pl.multiple_of((high * side + low) * PLANE, PLANE)
            plane = raw[:, pl.ds(start, PLANE)].astype(F32)
            for at in range(BLOCKS):
                row = (low * BLOCKS + at) * 8
                tiles[row : row + COMPS, :] = plane[:, at * LANES : (at + 1) * LANES]
            for comp in range(0, COMPS, 2):
                pieces = [
                    tiles[pl.ds(low * BLOCKS * 8 + c, BLOCKS, stride=8), :]
                    for c in (comp, comp + 1)
                ]
                blocks[high, low, comp * BLOCKS : (comp + 2) * BLOCKS, :] = jnp.concatenate(
                    pieces, axis=0
                ).astype(BF16)


def pack_links(links_ref, links_out, links_z_out):
    for at in range(BLOCKS):
        lanes = slice(at * LANES, (at + 1) * LANES)
        rows = [links_ref[direction, :, lanes].astype(F32) for direction in range(NDIR)]
        for direction in range(NDIR):
            links_out[at, direction * 24 : direction * 24 + 18, :] = rows[direction].astype(BF16)
        if at >= BLOCKS // 2:
            links_z_out[at - BLOCKS // 2, 0:18, :] = rows[2].astype(BF16)


def fill_tables(links, table):
    lane = lax.broadcasted_iota(jnp.int32, (1, LANES), 1)
    x_lane = jnp.bitwise_and(lane, LXY - 1)

    def block(index):
        return slice(index * LANES, (index + 1) * LANES)

    for direction in range(2):
        for at in range(BLOCKS):
            wide = 0.5 * links[at, direction * 24 : direction * 24 + 24, :].astype(F32)
            own = [wide[e : e + 1] for e in range(18)]
            if direction == 0:
                moved = [jnp.where(x_lane == 0, roll(u, 97), roll(u, 1)) for u in own]
            else:
                before = (at + BLOCKS - 1) % BLOCKS
                wide = 0.5 * links[before, direction * 24 : direction * 24 + 24, :].astype(F32)
                other = [wide[e : e + 1] for e in range(18)]
                moved = [
                    jnp.where(lane < LXY, roll(o, LXY), roll(u, LXY)) for o, u in zip(other, own)
                ]
            for e in range(18):
                table[2 * direction, e : e + 1, block(at)] = own[e]
            for e, value in enumerate(minus_adjoint(moved)):
                table[2 * direction + 1, e : e + 1, block(at)] = value


def fill_z_tables(links, links_z, table):
    for at in range(BLOCKS):
        lanes = slice(at * LANES, (at + 1) * LANES)
        if at < BLOCKS // 2:
            wide = 0.5 * links[at, 48:72, :].astype(F32)
            straight, turned = 4, 5
        else:
            wide = 0.5 * links_z[at - BLOCKS // 2, 0:24, :].astype(F32)
            straight, turned = 5, 4
        own = [wide[e : e + 1] for e in range(18)]
        for e in range(18):
            table[straight, e : e + 1, lanes] = own[e]
        for e, value in enumerate(minus_adjoint(own)):
            table[turned, e : e + 1, lanes] = value


def fill_order(core, side, order):
    bits = side.bit_length() - 1
    width = 2 * side * side
    row = lax.broadcasted_iota(jnp.int32, (width, width), 0)
    column = lax.broadcasted_iota(jnp.int32, (width, width), 1)
    low = jnp.bitwise_and(row, side - 1)
    place = jnp.bitwise_and(jnp.right_shift(row, bits), side - 1)
    rest = row - low - place * side
    high = jnp.right_shift(place, 1) + (side // 2) * jnp.bitwise_and(place, 1)
    number = jnp.where(core == 1, low * side + high, high * side + low)
    order[...] = jnp.where(column == rest + number, 1.0, 0.0)


def kernel(
    side, vectors_hbm, links_hbm, momenta_hbm, directions_hbm, out_ref,
    raw, tiles, x_ref, links_ref, momenta_ref, directions_ref,
    ra, rb, spread, field, field_b, halo, links_z_out, links, links_z, table, cosine, sine, order,
    twisted, twisted_h, twisted_h0, packed_xy, packed_z, packed_h, acc_xy, acc_z, send_xy, send_z, got_xy, got_z,
    sum_xy, sum_z, rows_out, rows_in,
    sem_i, ready, sem_a, sem_b, sem_h, sem_l, sem_r, sem_s,
):
    nev = side * side
    pairs = side // 2
    group = 2 * side
    me, core = lax.axis_index("space"), lax.axis_index("tm")
    high, low = me // side, me % side
    a = low + core * (high - low)
    b = high + core * (low - high)

    def device(at_a, at_b):
        return (1 - core) * (at_b * side + at_a) + core * (at_a * side + at_b)

    above = (me + 1) % nev
    below = (me + nev - 1) % nev

    barrier = pltpu.get_barrier_semaphore()

    def greet(target):
        pl.semaphore_signal(barrier, inc=1, device_id={"space": target}, device_id_type=MESH)

    beside_b = (device(a, (b + 1) % side), device(a, (b + side - 1) % side))
    for step in range(1, side):
        greet(device((a + step) % side, b))
    for target in (above, below) + beside_b:
        greet(target)
    sources = (vectors_hbm, links_hbm, momenta_hbm, directions_hbm)
    targets = (raw, links_ref, momenta_ref, directions_ref)
    inputs = [
        pltpu.make_async_copy(source, target, sem_i.at[index])
        for index, (source, target) in enumerate(zip(sources, targets))
    ]
    for copy in inputs:
        copy.start()
    inputs[0].wait()
    make_blocks(side, raw, tiles, x_ref)
    inputs[1].wait()
    pack_links(links_ref, links, links_z_out)
    pl.semaphore_wait(barrier, side - 1 + 4)

    def send(src, dst, sent, arrived, target):
        copy = pltpu.make_async_remote_copy(
            src_ref=src, dst_ref=dst, send_sem=sent, recv_sem=arrived,
            device_id={"space": target}, device_id_type=MESH,
        )
        copy.start()
        return copy

    far_a = sorted(range(1, side), key=lambda k: -min(k, side - k))
    own_pair = b % pairs

    for step in far_a:
        to_a = (a + step) % side

        @pl.when(core == 0)
        def _():
            send(x_ref.at[:, to_a], ra.at[a], sem_s.at[2], sem_a, device(to_a, b))

        @pl.when(core == 1)
        def _():
            send(x_ref.at[to_a], ra.at[a], sem_s.at[2], sem_a, device(to_a, b))

    links_copy = send(links_z_out, links_z, sem_s.at[1], sem_l, above)
    for to_b in range(side):
        ra[a, to_b] = x_ref[
            (1 - core) * to_b + core * a, (1 - core) * a + core * to_b
        ]
    inputs[2].wait()
    inputs[3].wait()
    fill_phases(momenta_ref, me, nev, cosine, sine)
    fill_order(core, side, order)
    fill_tables(links, table)

    for place in range(side // 2 - 1):
        for target in beside_b:
            pl.semaphore_signal(
                ready.at[place], inc=1, device_id={"space": target}, device_id_type=MESH
            )
        pl.semaphore_wait(ready.at[place], 2)

    wait_for(ra.at[pl.ds(0, side - 1)], sem_a)
    for turn in reversed(range(pairs)):
        for member in range(2 if turn else 1):
            to_b = (b + turn) % pairs + member * pairs if turn else (b + pairs) % side
            send(ra.at[:, to_b], rb.at[b], sem_s.at[3], sem_b.at[own_pair], device(a, to_b))
    for from_a in range(side):
        rb[b, from_a] = ra[from_a, b]

    links_copy.wait()
    fill_z_tables(links, links_z, table)
    upper = pl.ds(HALF, HALF)
    lane = lax.broadcasted_iota(jnp.int32, (1, LANES), 1)
    x_lane = jnp.bitwise_and(lane, LXY - 1)
    lower_half = pl.ds(0, HALF)

    def own_arrive(pair):
        @pl.when(pair == own_pair)
        def _():
            wait_for(rb.at[pl.ds(0, 1)], sem_b.at[pair])

        @pl.when(pair != own_pair)
        def _():
            wait_for(rb.at[pl.ds(0, 2)], sem_b.at[pair])

        for member in range(2):
            for from_a in range(side):
                spread[pl.ds((member * side + from_a) * PITCH, BLOCK_ROWS), :] = rb[
                    pair + member * pairs, from_a
                ].astype(F32)
        for comp in range(COMPS):
            for at in range(BLOCKS):
                rows = spread[pl.ds(comp * BLOCKS + at, group, stride=PITCH), :]
                field[comp, :, at * LANES : (at + 1) * LANES] = rows
                field_b[pair, comp, :, at * LANES : (at + 1) * LANES] = rows.astype(BF16)
        send(
            field_b.at[pair, :, :, lower_half], halo.at[pair, :, :, lower_half],
            sem_s.at[4], sem_h.at[0, pair], below,
        )
        send(
            field_b.at[pair, :, :, upper], halo.at[pair, :, :, upper],
            sem_s.at[4], sem_h.at[1, pair], above,
        )


    def own_block(pair, at):
        rows_at = pl.multiple_of(pair * group, group)
        lanes = lanes_at(0, at)
        after = lanes_at(0, (at + 1) % BLOCKS)
        before = lanes_at(0, (at + BLOCKS - 1) % BLOCKS)
        vec = [field[c, :, lanes] for c in range(COMPS)]
        store_twisted(twisted, pair, group, at, cosine.at[0], sine.at[0], vec)
        ahead = [jnp.where(x_lane == LXY - 1, roll(v, 31), roll(v, 127)) for v in vec]
        behind = [jnp.where(x_lane == 0, roll(v, 97), roll(v, 1)) for v in vec]
        first = apply_table(table.at[0], lanes, ahead)
        second = apply_table(table.at[1], lanes, behind)
        store_packed(
            packed_xy, 0, 0, nev, rows_at, group, at, [f + s for f, s in zip(first, second)]
        )
        ahead = [
            jnp.where(lane < LANES - LXY, roll(v, 96), roll(field[c, :, after], 96))
            for c, v in enumerate(vec)
        ]
        behind = [
            jnp.where(lane < LXY, roll(field[c, :, before], LXY), roll(v, LXY))
            for c, v in enumerate(vec)
        ]
        first = apply_table(table.at[2], lanes, ahead)
        second = apply_table(table.at[3], lanes, behind)
        store_packed(
            packed_xy, 2 * nev, 0, nev, rows_at, group, at,
            [f + s for f, s in zip(first, second)],
        )
        store_packed(
            packed_h, 0, 0, nev, rows_at, group, at,
            apply_table(table.at[5], lanes, vec),
        )

    def own_plane(pair):
        own_arrive(pair)

        @pl.loop(0, BLOCKS)
        def _(at):
            own_block(pair, at)

    def halo_wait(which):
        for pair in which:
            wait_for(halo.at[0, :, :, lower_half], sem_h.at[0, pair])
            wait_for(halo.at[0, :, :, upper], sem_h.at[1, pair])

    def beside_block(target, place, pair, at):
        rows_at = pair * group
        lanes = lanes_at(0, at)
        vec = [halo[pair, c, :, lanes].astype(F32) for c in range(COMPS)]
        store_twisted(target, place, group, at, cosine.at[1], sine.at[1], vec)
        store_packed(
            packed_z, 0, 0, nev, rows_at, group, at, apply_table(table.at[4], lanes, vec)
        )

    def spread_sums(acc, parts, outgoing, got, sent, sem):
        width = 2 * NMOM
        for to_a in range(side):
            for index in range(parts):
                for pair in range(pairs):
                    at = (index * pairs + pair) * width
                    outgoing[to_a, at : at + width, :] = acc[
                        index, pl.ds(pair * NMOM * group + to_a, width, stride=side), :
                    ].astype(BF16)
        for step in far_a:
            to_a = (a + step) % side
            send(outgoing.at[to_a], got.at[step - 1], sent, sem, device(to_a, b))

    def collect_sums(outgoing, got, total, sem):
        wait_for(got, sem)
        value = outgoing[a].astype(F32)
        for index in range(side - 1):
            value = value + got[index].astype(F32)
        total[...] = value

    for index in range(pairs - 1):
        own_plane(1 + (index + own_pair) % (pairs - 1))
    own_plane(0)

    product = contract(twisted[...], packed_xy[...])
    for index in range(2):
        acc_xy[index] = product[:, index * 2 * nev : (index + 1) * 2 * nev]
    halo_wait(range(1, pairs))

    @pl.loop(0, BLOCKS)
    def _(at):
        for pair in range(1, pairs):
            beside_block(twisted_h, pair - 1, pair, at)

    spread_sums(acc_xy, 2, send_xy, got_xy, sem_s.at[5], sem_r.at[0])
    early = slice(NMOM * group, NMOM * nev)
    late = slice(0, NMOM * group)
    acc_z[0, early, :] = contract(twisted_h[...], packed_h[...])
    halo_wait([0])

    @pl.loop(0, BLOCKS)
    def _(at):
        beside_block(twisted_h0, 0, 0, at)

    acc_z[0, late, :] = contract(twisted_h0[...], packed_h[...])
    acc_z[0] += contract(twisted[...], packed_z[...])
    spread_sums(acc_z, 1, send_z, got_z, sem_s.at[6], sem_r.at[1])

    collect_sums(send_xy, got_xy, sum_xy, sem_r.at[0])
    collect_sums(send_z, got_z, sum_z, sem_r.at[1])
    for place in range(side):
        first = (place // 2) * 2 * NMOM + place % 2
        for index, total in enumerate((sum_xy, sum_xy, sum_z)):
            start = first + (index % 2) * NMOM * side
            rows_out[place, index * NMOM : (index + 1) * NMOM, :] = total[
                pl.ds(start, NMOM, stride=2), :
            ]

    def place_of(at_b):
        return 2 * (at_b % pairs) + at_b // pairs

    for step in far_a:
        to_b = (b + step) % side
        send(rows_out.at[place_of(to_b)], rows_in.at[step - 1], sem_s.at[7], sem_r.at[2], device(a, to_b))
    wait_for(rows_in, sem_r.at[2])
    value = rows_out[place_of(b)]
    for index in range(side - 1):
        value = value + rows_in[index]
    last = jnp.dot(value, order[...], preferred_element_type=F32, precision=lax.Precision.HIGHEST)
    by_dir = [last[index * NMOM : (index + 1) * NMOM] for index in range(NDIR)]
    for slot in range(NDIR):
        chosen = directions_ref[slot]
        out_ref[slot] = jnp.where(
            chosen == 0, by_dir[0], jnp.where(chosen == 1, by_dir[1], by_dir[2])
        )

    wait_for(ra.at[pl.ds(0, side - 1)], sem_s.at[2])
    wait_for(rb.at[pl.ds(0, side - 1)], sem_s.at[3])
    wait_for(field_b, sem_s.at[4])
    wait_for(got_xy, sem_s.at[5])
    wait_for(got_z, sem_s.at[6])
    wait_for(rows_in, sem_s.at[7])


def shards(vectors, gauge_links, momenta, directions):
    space = lax.axis_size("space")
    side = math.isqrt(space)
    nev, pairs, group = space, side // 2, 2 * side
    scratch = [
        ((COMPS, space * PLANE), BF16),
        ((side * BLOCKS * 8, LANES), F32),
        ((side, side, BLOCK_ROWS, LANES), BF16),
        ((NDIR, 18, PLANE), BF16),
        ((side, side, BLOCK_ROWS, LANES), BF16),
        ((side, side, BLOCK_ROWS, LANES), BF16),
        ((group * PITCH, LANES), F32),
        ((COMPS, group, PLANE), F32),
        ((pairs, COMPS, group, PLANE), BF16),
        ((pairs, COMPS, group, PLANE), BF16),
        ((BLOCKS // 2, 32, LANES), BF16),
        ((BLOCKS, 80, LANES), BF16),
        ((BLOCKS // 2, 32, LANES), BF16),
        ((6, 24, PLANE), F32),
        ((2, NMOM, PLANE), F32),
        ((2, NMOM, PLANE), F32),
        ((2 * nev, 2 * nev), F32),
        ((NMOM * nev, DEPTH), BF16),
        ((NMOM * (nev - group), DEPTH), BF16),
        ((NMOM * group, DEPTH), BF16),
        ((4 * nev, DEPTH), BF16),
        ((2 * nev, DEPTH), BF16),
        ((2 * nev, DEPTH), BF16),
        ((2, NMOM * nev, 2 * nev), F32),
        ((1, NMOM * nev, 2 * nev), F32),
        ((side, 2 * NMOM * side, 2 * nev), BF16),
        ((side, NMOM * side, 2 * nev), BF16),
        ((side - 1, 2 * NMOM * side, 2 * nev), BF16),
        ((side - 1, NMOM * side, 2 * nev), BF16),
        ((2 * NMOM * side, 2 * nev), F32),
        ((NMOM * side, 2 * nev), F32),
        ((side, NDIR * NMOM, 2 * nev), F32),
        ((side - 1, NDIR * NMOM, 2 * nev), F32),
    ]
    dma = pltpu.SemaphoreType.DMA
    out = pl.pallas_call(
        functools.partial(kernel, side),
        out_shape=jax.ShapeDtypeStruct((NDIR, NMOM, 2 * nev), F32),
        in_specs=[pl.BlockSpec(memory_space=pl.ANY)] * 4,
        out_specs=pl.BlockSpec(memory_space=pltpu.VMEM),
        scratch_shapes=[pltpu.VMEM(*s) for s in scratch[:4]]
        + [pltpu.SMEM((NDIR, NMOM), jnp.int32), pltpu.SMEM((NDIR,), jnp.int32)]
        + [pltpu.VMEM(*s) for s in scratch[4:]]
        + [dma((4,))]
        + [pltpu.SemaphoreType.REGULAR((max(1, side // 2 - 1),))]
        + [dma, dma((pairs,)), dma((2, pairs)), dma, dma((3,)), dma((8,))],
        compiler_params=pltpu.CompilerParams(
            collective_id=0, has_side_effects=True, vmem_limit_bytes=60 * 1024 * 1024
        ),
    )(vectors[0, 0], gauge_links[0], momenta.T, directions)
    return jnp.transpose(out, (1, 0, 2))[None, None]


def solution(mesh):
    return jax.shard_map(
        shards,
        mesh=mesh,
        in_specs=(
            P(("cfg", "tm"), "space", None, None),
            P(("cfg", "tm"), None, None, "space"),
            P(),
            P(),
        ),
        out_specs=P("space", ("cfg", "tm"), None, None, None),
        check_vma=False,
    )
```

```python
import functools
import math

import jax
import jax.numpy as jnp
from jax import lax
from jax.experimental import pallas as pl
from jax.experimental.pallas import tpu as pltpu
from jax.sharding import PartitionSpec as P

LXY = 32
NMOM = 8
NDIR = 3
PLANE = LXY * LXY
LANES = 128
BLOCKS = PLANE // LANES
HALF = PLANE // 2
COMPS = 6
BLOCK_ROWS = COMPS * BLOCKS
PITCH = BLOCK_ROWS + 8
DEPTH = COMPS * PLANE
TWO_PI = 2.0 * math.pi
MESH = pl.DeviceIdType.MESH
BF16, F32 = jnp.bfloat16, jnp.float32


def roll(value, shift):
    return pltpu.roll(value, shift, value.ndim - 1)


def apply_table(table, lanes, field):
    out_re, out_im = [], []
    for row in range(3):
        acc_re = acc_im = None
        for col in range(3):
            link_re = table[3 * row + col : 3 * row + col + 1, lanes]
            link_im = table[9 + 3 * row + col : 10 + 3 * row + col, lanes]
            re = link_re * field[col] - link_im * field[3 + col]
            im = link_re * field[3 + col] + link_im * field[col]
            acc_re = re if acc_re is None else acc_re + re
            acc_im = im if acc_im is None else acc_im + im
        out_re.append(acc_re)
        out_im.append(acc_im)
    return out_re + out_im


def minus_adjoint(entries):
    real = [-entries[3 * b + a] for a in range(3) for b in range(3)]
    imag = [entries[9 + 3 * b + a] for a in range(3) for b in range(3)]
    return real + imag


def lanes_at(slot, at):
    return pl.ds(pl.multiple_of(slot * PLANE + at * LANES, LANES), LANES)


def store_packed(packed, base, first, nev, rows_at, group, at, value):
    for colour in range(3):
        re = value[colour].astype(BF16)
        im = value[3 + colour].astype(BF16)
        upper, lower = pl.ds(base + rows_at, group), pl.ds(base + nev + rows_at, group)
        packed[upper, lanes_at(first + colour, at)] = re
        packed[lower, lanes_at(first + colour, at)] = im
        packed[upper, lanes_at(first + 3 + colour, at)] = im
        packed[lower, lanes_at(first + 3 + colour, at)] = -re


def store_twisted(twisted, pair, group, at, cosine, sine, field):
    for mom in range(NMOM):
        cos_row = cosine[mom : mom + 1, lanes_at(0, at)]
        sin_row = sine[mom : mom + 1, lanes_at(0, at)]
        rows = pl.ds(pl.multiple_of(pair * NMOM * group, group) + mom * group, group)
        for colour in range(3):
            vec_re, vec_im = field[colour], field[3 + colour]
            twisted[rows, lanes_at(colour, at)] = (
                vec_re * cos_row - vec_im * sin_row
            ).astype(BF16)
            twisted[rows, lanes_at(3 + colour, at)] = (
                vec_re * sin_row + vec_im * cos_row
            ).astype(BF16)


def contract(left, right):
    return lax.dot_general(left, right, (((1,), (1,)), ((), ())), preferred_element_type=F32)


def wait_for(ref, sem):
    pltpu.make_async_copy(ref, ref, sem).wait()


def fill_phases(momenta, plane, z_length, cosine, sine):
    row = lax.broadcasted_iota(jnp.int32, (NMOM, LANES), 0)
    lane = lax.broadcasted_iota(jnp.int32, (NMOM, LANES), 1)

    def column(axis):
        value = jnp.zeros((NMOM, LANES), jnp.int32)
        for mom in range(NMOM):
            value = jnp.where(row == mom, momenta[axis, mom], value)
        return value

    mom_x, mom_y, mom_z = column(0), column(1), column(2)
    part_x = jnp.bitwise_and(mom_x * jnp.bitwise_and(lane, LXY - 1), LXY - 1).astype(F32) / LXY
    y_low = jnp.right_shift(lane, LXY.bit_length() - 1)
    for at in range(BLOCKS):
        y_coord = y_low + at * (LANES // LXY)
        part_y = jnp.bitwise_and(mom_y * y_coord, LXY - 1).astype(F32) / LXY
        beside = plane + 1 if at < BLOCKS // 2 else plane + z_length - 1
        for index, z_coord in enumerate((plane, beside)):
            part_z = jnp.bitwise_and(mom_z * z_coord, z_length - 1).astype(F32) / z_length
            theta = TWO_PI * (part_x + part_y + part_z)
            cosine[index, :, at * LANES : (at + 1) * LANES] = jnp.cos(theta)
            sine[index, :, at * LANES : (at + 1) * LANES] = jnp.sin(theta)


def make_blocks(side, raw, tiles, blocks):
    @pl.loop(0, side)
    def _(high):
        for low in range(side):
            start = pl.multiple_of((high * side + low) * PLANE, PLANE)
            plane = raw[:, pl.ds(start, PLANE)].astype(F32)
            for at in range(BLOCKS):
                row = (low * BLOCKS + at) * 8
                tiles[row : row + COMPS, :] = plane[:, at * LANES : (at + 1) * LANES]
            for comp in range(0, COMPS, 2):
                pieces = [
                    tiles[pl.ds(low * BLOCKS * 8 + c, BLOCKS, stride=8), :]
                    for c in (comp, comp + 1)
                ]
                blocks[high, low, comp * BLOCKS : (comp + 2) * BLOCKS, :] = jnp.concatenate(
                    pieces, axis=0
                ).astype(BF16)


def pack_links(links_ref, links_out, links_z_out):
    for at in range(BLOCKS):
        lanes = slice(at * LANES, (at + 1) * LANES)
        rows = [links_ref[direction, :, lanes].astype(F32) for direction in range(NDIR)]
        for direction in range(NDIR):
            links_out[at, direction * 24 : direction * 24 + 18, :] = rows[direction].astype(BF16)
        if at >= BLOCKS // 2:
            links_z_out[at - BLOCKS // 2, 0:18, :] = rows[2].astype(BF16)


def fill_tables(links, table):
    lane = lax.broadcasted_iota(jnp.int32, (1, LANES), 1)
    x_lane = jnp.bitwise_and(lane, LXY - 1)

    def block(index):
        return slice(index * LANES, (index + 1) * LANES)

    for direction in range(2):
        for at in range(BLOCKS):
            wide = 0.5 * links[at, direction * 24 : direction * 24 + 24, :].astype(F32)
            own = [wide[e : e + 1] for e in range(18)]
            if direction == 0:
                moved = [jnp.where(x_lane == 0, roll(u, 97), roll(u, 1)) for u in own]
            else:
                before = (at + BLOCKS - 1) % BLOCKS
                wide = 0.5 * links[before, direction * 24 : direction * 24 + 24, :].astype(F32)
                other = [wide[e : e + 1] for e in range(18)]
                moved = [
                    jnp.where(lane < LXY, roll(o, LXY), roll(u, LXY)) for o, u in zip(other, own)
                ]
            for e in range(18):
                table[2 * direction, e : e + 1, block(at)] = own[e]
            for e, value in enumerate(minus_adjoint(moved)):
                table[2 * direction + 1, e : e + 1, block(at)] = value


def fill_z_tables(links, links_z, table):
    for at in range(BLOCKS):
        lanes = slice(at * LANES, (at + 1) * LANES)
        if at < BLOCKS // 2:
            wide = 0.5 * links[at, 48:72, :].astype(F32)
            straight, turned = 4, 5
        else:
            wide = 0.5 * links_z[at - BLOCKS // 2, 0:24, :].astype(F32)
            straight, turned = 5, 4
        own = [wide[e : e + 1] for e in range(18)]
        for e in range(18):
            table[straight, e : e + 1, lanes] = own[e]
        for e, value in enumerate(minus_adjoint(own)):
            table[turned, e : e + 1, lanes] = value


def fill_order(core, side, order):
    bits = side.bit_length() - 1
    width = 2 * side * side
    row = lax.broadcasted_iota(jnp.int32, (width, width), 0)
    column = lax.broadcasted_iota(jnp.int32, (width, width), 1)
    low = jnp.bitwise_and(row, side - 1)
    place = jnp.bitwise_and(jnp.right_shift(row, bits), side - 1)
    rest = row - low - place * side
    high = jnp.right_shift(place, 1) + (side // 2) * jnp.bitwise_and(place, 1)
    number = jnp.where(core == 1, low * side + high, high * side + low)
    order[...] = jnp.where(column == rest + number, 1.0, 0.0)


def kernel(
    side, vectors_hbm, links_hbm, momenta_hbm, directions_hbm, out_ref,
    raw, tiles, x_ref, links_ref, momenta_ref, directions_ref,
    ra, rb, spread, field, field_b, halo, links_z_out, links, links_z, table, cosine, sine, order,
    twisted, twisted_h, twisted_h0, packed_xy, packed_z, packed_h, acc_xy, acc_z, send_xy, send_z, got_xy, got_z,
    sum_xy, sum_z, rows_out, rows_in,
    sem_i, ready, sem_a, sem_b, sem_h, sem_l, sem_r, sem_s,
):
    nev = side * side
    pairs = side // 2
    group = 2 * side
    me, core = lax.axis_index("space"), lax.axis_index("tm")
    high, low = me // side, me % side
    a = low + core * (high - low)
    b = high + core * (low - high)

    def device(at_a, at_b):
        return (1 - core) * (at_b * side + at_a) + core * (at_a * side + at_b)

    above = (me + 1) % nev
    below = (me + nev - 1) % nev

    barrier = pltpu.get_barrier_semaphore()

    def greet(target):
        pl.semaphore_signal(barrier, inc=1, device_id={"space": target}, device_id_type=MESH)

    beside_b = (device(a, (b + 1) % side), device(a, (b + side - 1) % side))
    for step in range(1, side):
        greet(device((a + step) % side, b))
    for target in (above, below) + beside_b:
        greet(target)
    sources = (vectors_hbm, links_hbm, momenta_hbm, directions_hbm)
    targets = (raw, links_ref, momenta_ref, directions_ref)
    inputs = [
        pltpu.make_async_copy(source, target, sem_i.at[index])
        for index, (source, target) in enumerate(zip(sources, targets))
    ]
    for copy in inputs:
        copy.start()
    inputs[0].wait()
    make_blocks(side, raw, tiles, x_ref)
    inputs[1].wait()
    pack_links(links_ref, links, links_z_out)
    pl.semaphore_wait(barrier, side - 1 + 4)

    def send(src, dst, sent, arrived, target):
        copy = pltpu.make_async_remote_copy(
            src_ref=src, dst_ref=dst, send_sem=sent, recv_sem=arrived,
            device_id={"space": target}, device_id_type=MESH,
        )
        copy.start()
        return copy

    far_a = sorted(range(1, side), key=lambda k: -min(k, side - k))
    own_pair = b % pairs

    for step in far_a:
        to_a = (a + step) % side

        @pl.when(core == 0)
        def _():
            send(x_ref.at[:, to_a], ra.at[a], sem_s.at[2], sem_a, device(to_a, b))

        @pl.when(core == 1)
        def _():
            send(x_ref.at[to_a], ra.at[a], sem_s.at[2], sem_a, device(to_a, b))

    links_copy = send(links_z_out, links_z, sem_s.at[1], sem_l, above)
    for to_b in range(side):
        ra[a, to_b] = x_ref[
            (1 - core) * to_b + core * a, (1 - core) * a + core * to_b
        ]
    inputs[2].wait()
    inputs[3].wait()
    fill_phases(momenta_ref, me, nev, cosine, sine)
    fill_order(core, side, order)
    fill_tables(links, table)

    for place in range(side // 2 - 1):
        for target in beside_b:
            pl.semaphore_signal(
                ready.at[place], inc=1, device_id={"space": target}, device_id_type=MESH
            )
        pl.semaphore_wait(ready.at[place], 2)

    wait_for(ra.at[pl.ds(0, side - 1)], sem_a)
    for turn in reversed(range(pairs)):
        for member in range(2 if turn else 1):
            to_b = (b + turn) % pairs + member * pairs if turn else (b + pairs) % side
            send(ra.at[:, to_b], rb.at[b], sem_s.at[3], sem_b.at[own_pair], device(a, to_b))
    for from_a in range(side):
        rb[b, from_a] = ra[from_a, b]

    links_copy.wait()
    fill_z_tables(links, links_z, table)
    upper = pl.ds(HALF, HALF)
    lane = lax.broadcasted_iota(jnp.int32, (1, LANES), 1)
    x_lane = jnp.bitwise_and(lane, LXY - 1)
    lower_half = pl.ds(0, HALF)

    def own_arrive(pair):
        @pl.when(pair == own_pair)
        def _():
            wait_for(rb.at[pl.ds(0, 1)], sem_b.at[pair])

        @pl.when(pair != own_pair)
        def _():
            wait_for(rb.at[pl.ds(0, 2)], sem_b.at[pair])

        for member in range(2):
            for from_a in range(side):
                spread[pl.ds((member * side + from_a) * PITCH, BLOCK_ROWS), :] = rb[
                    pair + member * pairs, from_a
                ].astype(F32)
        for comp in range(COMPS):
            for at in range(BLOCKS):
                rows = spread[pl.ds(comp * BLOCKS + at, group, stride=PITCH), :]
                field[comp, :, at * LANES : (at + 1) * LANES] = rows
                field_b[pair, comp, :, at * LANES : (at + 1) * LANES] = rows.astype(BF16)
        send(
            field_b.at[pair, :, :, lower_half], halo.at[pair, :, :, lower_half],
            sem_s.at[4], sem_h.at[0, pair], below,
        )
        send(
            field_b.at[pair, :, :, upper], halo.at[pair, :, :, upper],
            sem_s.at[4], sem_h.at[1, pair], above,
        )


    def own_block(pair, at):
        rows_at = pl.multiple_of(pair * group, group)
        lanes = lanes_at(0, at)
        after = lanes_at(0, (at + 1) % BLOCKS)
        before = lanes_at(0, (at + BLOCKS - 1) % BLOCKS)
        vec = [field[c, :, lanes] for c in range(COMPS)]
        store_twisted(twisted, pair, group, at, cosine.at[0], sine.at[0], vec)
        ahead = [jnp.where(x_lane == LXY - 1, roll(v, 31), roll(v, 127)) for v in vec]
        behind = [jnp.where(x_lane == 0, roll(v, 97), roll(v, 1)) for v in vec]
        first = apply_table(table.at[0], lanes, ahead)
        second = apply_table(table.at[1], lanes, behind)
        store_packed(
            packed_xy, 0, 0, nev, rows_at, group, at, [f + s for f, s in zip(first, second)]
        )
        ahead = [
            jnp.where(lane < LANES - LXY, roll(v, 96), roll(field[c, :, after], 96))
            for c, v in enumerate(vec)
        ]
        behind = [
            jnp.where(lane < LXY, roll(field[c, :, before], LXY), roll(v, LXY))
            for c, v in enumerate(vec)
        ]
        first = apply_table(table.at[2], lanes, ahead)
        second = apply_table(table.at[3], lanes, behind)
        store_packed(
            packed_xy, 2 * nev, 0, nev, rows_at, group, at,
            [f + s for f, s in zip(first, second)],
        )
        store_packed(
            packed_h, 0, 0, nev, rows_at, group, at,
            apply_table(table.at[5], lanes, vec),
        )

    def own_plane(pair):
        own_arrive(pair)

        @pl.loop(0, BLOCKS)
        def _(at):
            own_block(pair, at)

    def halo_wait(which):
        for pair in which:
            wait_for(halo.at[0, :, :, lower_half], sem_h.at[0, pair])
            wait_for(halo.at[0, :, :, upper], sem_h.at[1, pair])

    def beside_block(target, place, pair, at):
        rows_at = pair * group
        lanes = lanes_at(0, at)
        vec = [halo[pair, c, :, lanes].astype(F32) for c in range(COMPS)]
        store_twisted(target, place, group, at, cosine.at[1], sine.at[1], vec)
        store_packed(
            packed_z, 0, 0, nev, rows_at, group, at, apply_table(table.at[4], lanes, vec)
        )

    def spread_sums(acc, parts, outgoing, got, sent, sem):
        width = 2 * NMOM
        for to_a in range(side):
            for index in range(parts):
                for pair in range(pairs):
                    at = (index * pairs + pair) * width
                    outgoing[to_a, at : at + width, :] = acc[
                        index, pl.ds(pair * NMOM * group + to_a, width, stride=side), :
                    ].astype(BF16)
        for step in far_a:
            to_a = (a + step) % side
            send(outgoing.at[to_a], got.at[step - 1], sent, sem, device(to_a, b))

    def collect_sums(outgoing, got, total, sem):
        wait_for(got, sem)
        value = outgoing[a].astype(F32)
        for index in range(side - 1):
            value = value + got[index].astype(F32)
        total[...] = value

    for index in range(pairs - 1):
        own_plane(1 + (index + own_pair) % (pairs - 1))
    own_plane(0)
    halo_wait(range(1, pairs))
    acc_xy[...] = jnp.zeros_like(acc_xy)

    def chunks(half):
        for slot in range(COMPS):
            yield pl.ds(pl.multiple_of(slot * PLANE + half * 2 * LANES, 2 * LANES), 2 * LANES)

    @pl.loop(0, BLOCKS // 2)
    def _(half):
        total = None
        for part in chunks(half):
            product = contract(twisted[:, part], packed_xy[:, part])
            total = product if total is None else total + product
        for index in range(2):
            acc_xy[index] += total[:, index * 2 * nev : (index + 1) * 2 * nev]
        for pair in range(1, pairs):
            for at in range(2):
                beside_block(twisted_h, pair - 1, pair, 2 * half + at)

    spread_sums(acc_xy, 2, send_xy, got_xy, sem_s.at[5], sem_r.at[0])
    early = slice(NMOM * group, NMOM * nev)
    late = slice(0, NMOM * group)
    acc_z[0, early, :] = contract(twisted_h[...], packed_h[...])
    halo_wait([0])

    @pl.loop(0, BLOCKS)
    def _(at):
        beside_block(twisted_h0, 0, 0, at)

    acc_z[0, late, :] = contract(twisted_h0[...], packed_h[...])
    acc_z[0] += contract(twisted[...], packed_z[...])
    spread_sums(acc_z, 1, send_z, got_z, sem_s.at[6], sem_r.at[1])

    collect_sums(send_xy, got_xy, sum_xy, sem_r.at[0])
    collect_sums(send_z, got_z, sum_z, sem_r.at[1])
    for place in range(side):
        first = (place // 2) * 2 * NMOM + place % 2
        for index, total in enumerate((sum_xy, sum_xy, sum_z)):
            start = first + (index % 2) * NMOM * side
            rows_out[place, index * NMOM : (index + 1) * NMOM, :] = total[
                pl.ds(start, NMOM, stride=2), :
            ]

    def place_of(at_b):
        return 2 * (at_b % pairs) + at_b // pairs

    for step in far_a:
        to_b = (b + step) % side
        send(rows_out.at[place_of(to_b)], rows_in.at[step - 1], sem_s.at[7], sem_r.at[2], device(a, to_b))
    wait_for(rows_in, sem_r.at[2])
    value = rows_out[place_of(b)]
    for index in range(side - 1):
        value = value + rows_in[index]
    last = jnp.dot(value, order[...], preferred_element_type=F32, precision=lax.Precision.HIGHEST)
    by_dir = [last[index * NMOM : (index + 1) * NMOM] for index in range(NDIR)]
    for slot in range(NDIR):
        chosen = directions_ref[slot]
        out_ref[slot] = jnp.where(
            chosen == 0, by_dir[0], jnp.where(chosen == 1, by_dir[1], by_dir[2])
        )

    wait_for(ra.at[pl.ds(0, side - 1)], sem_s.at[2])
    wait_for(rb.at[pl.ds(0, side - 1)], sem_s.at[3])
    wait_for(field_b, sem_s.at[4])
    wait_for(got_xy, sem_s.at[5])
    wait_for(got_z, sem_s.at[6])
    wait_for(rows_in, sem_s.at[7])


def shards(vectors, gauge_links, momenta, directions):
    space = lax.axis_size("space")
    side = math.isqrt(space)
    nev, pairs, group = space, side // 2, 2 * side
    scratch = [
        ((COMPS, space * PLANE), BF16),
        ((side * BLOCKS * 8, LANES), F32),
        ((side, side, BLOCK_ROWS, LANES), BF16),
        ((NDIR, 18, PLANE), BF16),
        ((side, side, BLOCK_ROWS, LANES), BF16),
        ((side, side, BLOCK_ROWS, LANES), BF16),
        ((group * PITCH, LANES), F32),
        ((COMPS, group, PLANE), F32),
        ((pairs, COMPS, group, PLANE), BF16),
        ((pairs, COMPS, group, PLANE), BF16),
        ((BLOCKS // 2, 32, LANES), BF16),
        ((BLOCKS, 80, LANES), BF16),
        ((BLOCKS // 2, 32, LANES), BF16),
        ((6, 24, PLANE), F32),
        ((2, NMOM, PLANE), F32),
        ((2, NMOM, PLANE), F32),
        ((2 * nev, 2 * nev), F32),
        ((NMOM * nev, DEPTH), BF16),
        ((NMOM * (nev - group), DEPTH), BF16),
        ((NMOM * group, DEPTH), BF16),
        ((4 * nev, DEPTH), BF16),
        ((2 * nev, DEPTH), BF16),
        ((2 * nev, DEPTH), BF16),
        ((2, NMOM * nev, 2 * nev), F32),
        ((1, NMOM * nev, 2 * nev), F32),
        ((side, 2 * NMOM * side, 2 * nev), BF16),
        ((side, NMOM * side, 2 * nev), BF16),
        ((side - 1, 2 * NMOM * side, 2 * nev), BF16),
        ((side - 1, NMOM * side, 2 * nev), BF16),
        ((2 * NMOM * side, 2 * nev), F32),
        ((NMOM * side, 2 * nev), F32),
        ((side, NDIR * NMOM, 2 * nev), F32),
        ((side - 1, NDIR * NMOM, 2 * nev), F32),
    ]
    dma = pltpu.SemaphoreType.DMA
    out = pl.pallas_call(
        functools.partial(kernel, side),
        out_shape=jax.ShapeDtypeStruct((NDIR, NMOM, 2 * nev), F32),
        in_specs=[pl.BlockSpec(memory_space=pl.ANY)] * 4,
        out_specs=pl.BlockSpec(memory_space=pltpu.VMEM),
        scratch_shapes=[pltpu.VMEM(*s) for s in scratch[:4]]
        + [pltpu.SMEM((NDIR, NMOM), jnp.int32), pltpu.SMEM((NDIR,), jnp.int32)]
        + [pltpu.VMEM(*s) for s in scratch[4:]]
        + [dma((4,))]
        + [pltpu.SemaphoreType.REGULAR((max(1, side // 2 - 1),))]
        + [dma, dma((pairs,)), dma((2, pairs)), dma, dma((3,)), dma((8,))],
        compiler_params=pltpu.CompilerParams(
            collective_id=0, has_side_effects=True, vmem_limit_bytes=60 * 1024 * 1024
        ),
    )(vectors[0, 0], gauge_links[0], momenta.T, directions)
    return jnp.transpose(out, (1, 0, 2))[None, None]


def solution(mesh):
    return jax.shard_map(
        shards,
        mesh=mesh,
        in_specs=(
            P(("cfg", "tm"), "space", None, None),
            P(("cfg", "tm"), None, None, "space"),
            P(),
            P(),
        ),
        out_specs=P("space", ("cfg", "tm"), None, None, None),
        check_vma=False,
    )
```
